32 devices in a mesh: pod: 2 (over x), dp: 4 (over z), sp: 4 (over y, core).
Axes of the slice: x: 2, y: 2, z: 4, core: 2. Of those that a mesh axis runs over, the one named last changes fastest.
Arguments:
- images: bfloat16 [128, 32, 168, 128], P(('pod', 'dp'), 'sp'), parts along dimension 0
- w_a: bfloat16 [1, 3, 3, 128, 128], replicated
- norm_a: float32 [1, 2, 128], replicated
- w_down: bfloat16 [3, 3, 128, 256], replicated
- norm_down: float32 [2, 256], replicated
- w_b: bfloat16 [3, 3, 3, 256, 256], replicated
- norm_b: float32 [3, 2, 256], replicated
Outputs:
- output: bfloat16 [128, 16, 84, 256], P(('pod', 'dp'), 'sp'), parts along dimension 0
There are 2 independent parts. The reference program is written for one: setup_inputs(seed, part) draws one part's arguments, and reference() takes and returns one part's arrays. A program takes and returns all parts, laid end to end along the dimension named above; an argument that names none is the same for every part.
All inputs are finite; a program needn't handle non-finite values.
Results may differ from the reference program's by a relative error of at most 0.00736.
Values are sent between devices in bfloat16 or wider.
A program may use at most 1 GiB of HBM per device.

```python
import jax
import jax.numpy as jnp
from jax import lax

BATCH = 64
HEIGHT = 32
WIDTH = 168
CH_A = 128
CH_B = 256
LAYERS_A = 1
LAYERS_B = 3
EPS_VALUE = 1e-5
CONV_DIMS = ('NHWC', 'HWIO', 'NHWC')


def setup_inputs(seed: int = 0, part: int = 0) -> dict:
    base_key = jax.random.key(seed)
    part_key = jax.random.fold_in(base_key, part)
    noise_key, dir_key, scale_key, offset_key, phase_key = jax.random.split(part_key, 5)
    weight_keys = jax.random.split(base_key, 9)
    row_pos = jnp.arange(HEIGHT, dtype=jnp.float32) * (2.0 / (HEIGHT - 1)) - 1.0
    row_col = row_pos[None, :, None, None]
    noise = jax.random.normal(noise_key, (BATCH, HEIGHT, WIDTH, CH_A), jnp.float32)
    chan_dir = jax.random.normal(dir_key, (BATCH, 1, 1, CH_A), jnp.float32)
    img_scale = jax.random.uniform(scale_key, (BATCH, 1, 1, 1), jnp.float32, 0.5, 1.5)
    img_offset = 0.5 * jax.random.normal(offset_key, (BATCH, 1, 1, CH_A), jnp.float32)
    phase = jax.random.uniform(phase_key, (BATCH, 1, 1, CH_A), jnp.float32, 0.0, 6.2831853)
    wave = 0.5 * jnp.sin(row_col * 7.0 + phase)
    x_val = img_scale * (0.7 * noise + row_col * chan_dir + wave) + img_offset
    w_a = jax.random.normal(weight_keys[0], (LAYERS_A, 3, 3, CH_A, CH_A), jnp.float32) * (9 * CH_A) ** -0.5
    norm_a = jnp.stack([jax.random.uniform(weight_keys[1], (LAYERS_A, CH_A), jnp.float32, 0.6, 1.4), 0.3 * jax.random.normal(weight_keys[2], (LAYERS_A, CH_A), jnp.float32)], axis=1)
    w_down = jax.random.normal(weight_keys[3], (3, 3, CH_A, CH_B), jnp.float32) * (9 * CH_A) ** -0.5
    norm_down = jnp.stack([jax.random.uniform(weight_keys[4], (CH_B,), jnp.float32, 0.6, 1.4), 0.3 * jax.random.normal(weight_keys[5], (CH_B,), jnp.float32)])
    w_b = jax.random.normal(weight_keys[6], (LAYERS_B, 3, 3, CH_B, CH_B), jnp.float32) * (9 * CH_B) ** -0.5
    norm_b = jnp.stack([jax.random.uniform(weight_keys[7], (LAYERS_B, CH_B), jnp.float32, 0.6, 1.4), 0.3 * jax.random.normal(weight_keys[8], (LAYERS_B, CH_B), jnp.float32)], axis=1)
    return {'images': x_val.astype(jnp.bfloat16), 'w_a': w_a.astype(jnp.bfloat16), 'norm_a': norm_a, 'w_down': w_down.astype(jnp.bfloat16), 'norm_down': norm_down, 'w_b': w_b.astype(jnp.bfloat16), 'norm_b': norm_b}


def conv_norm(hidden, weight, norm_pair, stride, pads):
    z_val = lax.conv_general_dilated(hidden.astype(jnp.float32), weight.astype(jnp.float32), (stride, stride), pads, dimension_numbers=CONV_DIMS)
    mean_val = jnp.mean(z_val, axis=(0, 1, 2))
    mean_sq = jnp.mean(z_val * z_val, axis=(0, 1, 2))
    inv_std = lax.rsqrt(mean_sq - mean_val * mean_val + EPS_VALUE)
    scaled = norm_pair[0] * (z_val - mean_val) * inv_std + norm_pair[1]
    return jnp.maximum(scaled, 0.0).astype(jnp.bfloat16)


def reference(images, w_a, norm_a, w_down, norm_down, w_b, norm_b):
    def same_step(hidden, layer_args):
        return conv_norm(hidden, layer_args[0], layer_args[1], 1, ((1, 1), (1, 1))), None
    hidden, unused_a = lax.scan(same_step, images, (w_a, norm_a))
    hidden = conv_norm(hidden, w_down, norm_down, 2, ((0, 1), (0, 1)))
    hidden, unused_b = lax.scan(same_step, hidden, (w_b, norm_b))
    return hidden
```

```python
import functools

import jax
import jax.numpy as jnp
from jax import lax
from jax.experimental import pallas as pl
from jax.experimental.pallas import tpu as pltpu
from jax.sharding import PartitionSpec as P

EPS_VALUE = 1e-5
MESH = pl.DeviceIdType.MESH
BF16 = jnp.bfloat16
F32 = jnp.float32


def stack_kernel(n_dp, n_sp, img, wa, na, wd, nd, wb, nb, out,
                 nat, stage, img_t, act_a, act_b, zbuf, zfin, out_nat,
                 wa_v, wd_v, wb_v, stat_src, stat_dst,
                 in_sem, w_sem, halo_in_send, halo_in_recv, stat_send, stat_recv,
                 halo_send, halo_recv, out_sem):
    n_img, n_row, width, ch_a = img.shape
    n_out_row, w_out, ch_b = out.shape[1], out.shape[2], out.shape[3]
    n_layers_b = wb.shape[0]
    n_group = n_dp * n_sp
    m_row = w_out * n_img
    my_pod, my_dp, my_sp = lax.axis_index("pod"), lax.axis_index("dp"), lax.axis_index("sp")
    me = my_dp * n_sp + my_sp
    is_top = my_sp == 0
    is_bottom = my_sp == n_sp - 1
    not_top = my_sp > 0
    not_bottom = my_sp < n_sp - 1
    upper = (my_pod, my_dp, lax.max(my_sp - 1, 0))
    lower = (my_pod, my_dp, lax.min(my_sp + 1, n_sp - 1))

    def peer(offset):
        flat = lax.rem(me + offset, n_group)
        return (my_pod, flat // n_sp, lax.rem(flat, n_sp))

    row_copies = [pltpu.make_async_copy(img.at[:, r], nat.at[r + 1], in_sem.at[r]) for r in range(n_row)]
    for c in row_copies:
        c.start()
    w_copies = []
    for p in range(3):
        for q in range(3):
            for half in range(2):
                k = q + half
                w_copies.append(pltpu.make_async_copy(
                    wa.at[p, q], wa_v.at[pl.ds(p * 4 * ch_a + k * ch_a, ch_a), pl.ds(half * ch_a, ch_a)],
                    w_sem.at[len(w_copies)]))
    for p in range(3):
        for q in range(3):
            off = p * 2 * ch_a + q * ch_a if q < 2 else 6 * ch_a + p * ch_a
            w_copies.append(pltpu.make_async_copy(wd.at[p, q], wd_v.at[pl.ds(off, ch_a)], w_sem.at[len(w_copies)]))
    w_copies.append(pltpu.make_async_copy(wb, wb_v, w_sem.at[len(w_copies)]))
    for c in w_copies:
        c.start()

    barrier = pltpu.get_barrier_semaphore()
    for i in range(1, n_group):
        pl.semaphore_signal(barrier, inc=1, device_id=peer(i), device_id_type=MESH)

    for p in range(3):
        wa_v[pl.ds(p * 4 * ch_a + 3 * ch_a, ch_a), 0:ch_a] = jnp.zeros((ch_a, ch_a), BF16)
        wa_v[pl.ds(p * 4 * ch_a, ch_a), ch_a:2 * ch_a] = jnp.zeros((ch_a, ch_a), BF16)
    n_rows_t = img_t.shape[0]
    img_t[:, 0, :, 0:ch_a] = jnp.zeros((n_rows_t, n_img, ch_a), BF16)
    img_t[:, w_out, :, ch_a:2 * ch_a] = jnp.zeros((n_rows_t, n_img, ch_a), BF16)
    act_a[:, w_out] = jnp.zeros((act_a.shape[0], n_img, 2 * ch_a), BF16)
    act_b[:, 0] = jnp.zeros((act_b.shape[0], n_img, ch_b), BF16)
    act_b[:, w_out + 1] = jnp.zeros((act_b.shape[0], n_img, ch_b), BF16)

    @pl.when(is_top)
    def _():
        nat[0] = jnp.zeros((n_img, width, ch_a), BF16)
        act_b[0] = jnp.zeros((w_out + 2, n_img, ch_b), BF16)

    @pl.when(is_bottom)
    def _():
        nat[n_row + 1] = jnp.zeros((n_img, width, ch_a), BF16)
        nat[n_row + 2] = jnp.zeros((n_img, width, ch_a), BF16)
        act_b[n_out_row + 1] = jnp.zeros((w_out + 2, n_img, ch_b), BF16)

    pl.semaphore_wait(barrier, n_group - 1)

    def image_halo(src_row, dst_row, dev, k):
        return pltpu.make_async_remote_copy(
            src_ref=img.at[:, src_row], dst_ref=nat.at[dst_row], send_sem=halo_in_send.at[k],
            recv_sem=halo_in_recv.at[k], device_id=dev, device_id_type=MESH)

    to_lower = image_halo(n_row - 1, 0, lower, 0)
    to_upper0 = image_halo(0, n_row + 1, upper, 1)
    to_upper1 = image_halo(1, n_row + 2, upper, 2)

    @pl.when(not_bottom)
    def _():
        to_lower.start()

    @pl.when(not_top)
    def _():
        to_upper0.start()
        to_upper1.start()

    def transpose_row(k):
        pitch = stage.shape[0] // n_img

        for i in range(n_img):
            stage[pl.ds(i * pitch, width), :] = nat[k, i].astype(F32)
        for x in range(width):
            half = (x + 1) % 2
            img_t[k, (x + 1) // 2, :, half * ch_a:(half + 1) * ch_a] = (
                stage[pl.ds(x, n_img, stride=pitch), :].astype(BF16))

    def fold(total, z_val):
        z3 = z_val.reshape(m_row // 8, 8, ch_b)
        return total[0] + jnp.sum(z3, axis=0), total[1] + jnp.sum(z3 * z3, axis=0)

    def conv_a(r):
        parts = []
        for p in range(3):
            for k in range(2):
                parts.append(img_t[r + p, pl.ds(k, w_out)].reshape(m_row, 2 * ch_a))
        return jnp.dot(jnp.concatenate(parts, axis=1), wa_v[...], preferred_element_type=F32)

    def conv_down(r):
        parts = [act_a[2 * r + p, pl.ds(0, w_out)].reshape(m_row, 2 * ch_a) for p in range(3)]
        parts += [act_a[2 * r + p, pl.ds(1, w_out), :, 0:ch_a].reshape(m_row, ch_a) for p in range(3)]
        return jnp.dot(jnp.concatenate(parts, axis=1), wd_v[...], preferred_element_type=F32)

    def conv_b(r, layer):
        parts = []
        for p in range(3):
            for q in range(3):
                parts.append(act_b[r + p, pl.ds(q, w_out)].reshape(m_row, ch_b))
        return jnp.dot(jnp.concatenate(parts, axis=1), wb_v[layer], preferred_element_type=F32)

    def run_rows(rows, conv, total, keep):
        first, step, count = rows

        def body(i, total):
            r = first + i * step
            z_val = conv(r)
            keep(r, z_val)
            return fold(total, z_val)

        return lax.fori_loop(0, count, body, total)

    def keep_z(r, z_val):
        zbuf[r] = z_val

    def keep_final(r, z_val):
        pitch = zfin.shape[1] // (n_out_row * w_out)
        for x in range(w_out):
            for h in range(ch_b // 128):
                zfin[h, pl.ds((r * w_out + x) * pitch, n_img), :] = z_val[x * n_img:(x + 1) * n_img, h * 128:(h + 1) * 128]

    def send_stats(layer, total):
        s1 = jnp.sum(total[0], axis=0, keepdims=True)
        s2 = jnp.sum(total[1], axis=0, keepdims=True)
        if layer == 0:
            s1 = s1[:, :ch_a] + s1[:, ch_a:]
            s2 = s2[:, :ch_a] + s2[:, ch_a:]
            s1 = jnp.concatenate([s1, s1], axis=1)
            s2 = jnp.concatenate([s2, s2], axis=1)
        both = jnp.concatenate([s1, s2], axis=0)
        stat_src[layer] = both
        stat_dst[layer, me] = both
        copies = []
        for i in range(1, n_group):
            copies.append(pltpu.make_async_remote_copy(
                src_ref=stat_src.at[layer], dst_ref=stat_dst.at[layer, me], send_sem=stat_send.at[layer, i],
                recv_sem=stat_recv.at[layer, i], device_id=peer(i), device_id_type=MESH))
        for c in copies:
            c.start()
        return copies

    def finish_stats(layer, copies, gamma, beta, count):
        for c in copies:
            c.wait()
        tot = jnp.sum(stat_dst[layer], axis=0)
        mean = tot[0:1] / count
        var = tot[1:2] / count - mean * mean
        scale = gamma * lax.rsqrt(var + EPS_VALUE)
        return mean, scale, beta

    def normalize(z_val, coef):
        mean, scale, beta = coef
        return jnp.maximum((z_val - mean) * scale + beta, 0.0).astype(BF16)

    zeros = (jnp.zeros((8, ch_b), F32), jnp.zeros((8, ch_b), F32))

    for c in row_copies:
        c.wait()

    def t_body(k, carry):
        transpose_row(k)
        return carry

    lax.fori_loop(1, n_row + 1, t_body, 0)
    for c in w_copies:
        c.wait()
    total = run_rows((1, 1, n_row - 2), conv_a, zeros, keep_z)

    @pl.when(not_top)
    def _():
        to_lower.wait_recv()

    @pl.when(not_bottom)
    def _():
        to_upper0.wait_recv()
        to_upper1.wait_recv()

    def t_body_halo(k, carry):
        transpose_row(jnp.where(k == 0, 0, n_row + k))
        return carry

    lax.fori_loop(0, 3, t_body_halo, 0)
    total = run_rows((0, n_row - 1, 2), conv_a, total, keep_z)
    copies = send_stats(0, total)
    zbuf[n_row] = conv_a(n_row)
    n_a = float(n_group * n_img * n_row * width)
    wide = lambda v: jnp.concatenate([v, v], axis=1)
    coef = finish_stats(0, copies, wide(na[0, 0:1]), wide(na[0, 1:2]), n_a)

    def norm_a_body(r, carry):
        act_a[r, pl.ds(0, w_out)] = normalize(zbuf[r], coef).reshape(w_out, n_img, 2 * ch_a)
        return carry

    lax.fori_loop(0, n_row + 1, norm_a_body, 0)

    @pl.when(is_bottom)
    def _():
        act_a[n_row] = jnp.zeros((w_out + 1, n_img, 2 * ch_a), BF16)

    total = run_rows((0, 1, n_out_row), conv_down, zeros, keep_z)
    copies = send_stats(1, total)
    n_b = float(n_group * m_row * n_out_row)
    coef = finish_stats(1, copies, nd[0:1], nd[1:2], n_b)

    for layer in range(n_layers_b):
        def norm_b_row(r):
            act_b[r + 1, pl.ds(1, w_out)] = normalize(zbuf[r], coef).reshape(w_out, n_img, ch_b)

        down = pltpu.make_async_remote_copy(
            src_ref=act_b.at[n_out_row, pl.ds(1, w_out)], dst_ref=act_b.at[0, pl.ds(1, w_out)],
            send_sem=halo_send.at[layer, 0], recv_sem=halo_recv.at[layer, 0], device_id=lower, device_id_type=MESH)
        up = pltpu.make_async_remote_copy(
            src_ref=act_b.at[1, pl.ds(1, w_out)], dst_ref=act_b.at[n_out_row + 1, pl.ds(1, w_out)],
            send_sem=halo_send.at[layer, 1], recv_sem=halo_recv.at[layer, 1], device_id=upper, device_id_type=MESH)

        norm_b_row(0)

        @pl.when(not_top)
        def _():
            up.start()

        norm_b_row(n_out_row - 1)

        @pl.when(not_bottom)
        def _():
            down.start()

        def norm_b_body(r, carry):
            norm_b_row(r)
            return carry

        lax.fori_loop(1, n_out_row - 1, norm_b_body, 0)
        last = layer == n_layers_b - 1
        conv = functools.partial(conv_b, layer=layer)
        keep = keep_final if last else keep_z
        total = run_rows((1, 1, n_out_row - 2), conv, zeros, keep)

        @pl.when(not_top)
        def _():
            up.wait_send()
            down.wait_recv()

        @pl.when(not_bottom)
        def _():
            down.wait_send()
            up.wait_recv()

        total = run_rows((0, n_out_row - 1, 2), conv, total, keep)
        copies = send_stats(2 + layer, total)
        coef = finish_stats(2 + layer, copies, nb[layer, 0:1], nb[layer, 1:2], n_b)

    pitch = zfin.shape[1] // (n_out_row * w_out)

    def out_body(r, carry):
        for i in range(n_img):
            for h in range(ch_b // 128):
                lanes = slice(h * 128, (h + 1) * 128)
                z_val = zfin[h, pl.ds(r * w_out * pitch + i, w_out, stride=pitch), :]
                out_nat[r, i, :, lanes] = normalize(z_val, tuple(v[:, lanes] for v in coef))
        pltpu.make_async_copy(out_nat.at[r], out.at[:, r], out_sem.at[r]).start()
        return carry

    lax.fori_loop(0, n_out_row, out_body, 0)
    for r in range(n_out_row):
        pltpu.make_async_copy(out_nat.at[r], out.at[:, r], out_sem.at[r]).wait()

    @pl.when(not_bottom)
    def _():
        to_lower.wait_send()

    @pl.when(not_top)
    def _():
        to_upper0.wait_send()
        to_upper1.wait_send()


def solution(mesh):
    n_sp, n_dp = mesh.shape['sp'], mesh.shape['dp']

    def local_stack(img, w_a, norm_a, w_down, norm_down, w_b, norm_b):
        n_img, n_row, width, ch_a = img.shape
        ch_b = w_down.shape[-1]
        n_out_row, w_out = n_row // 2, width // 2
        n_layers_b = w_b.shape[0]
        n_group = n_sp * n_dp
        any_spec = pl.BlockSpec(memory_space=pl.ANY)
        vmem_spec = pl.BlockSpec(memory_space=pltpu.VMEM)
        dma = pltpu.SemaphoreType.DMA
        n_stats = 2 + n_layers_b
        return pl.pallas_call(
            functools.partial(stack_kernel, n_dp, n_sp),
            out_shape=jax.ShapeDtypeStruct((n_img, n_out_row, w_out, ch_b), BF16),
            in_specs=[any_spec, any_spec, vmem_spec, any_spec, vmem_spec, any_spec, vmem_spec],
            out_specs=any_spec,
            scratch_shapes=[
                pltpu.VMEM((n_row + 3, n_img, width, ch_a), BF16),
                pltpu.VMEM((n_img * width, 128), F32),
                pltpu.VMEM((n_row + 3, w_out + 1, n_img, 2 * ch_a), BF16),
                pltpu.VMEM((n_row + 1, w_out + 1, n_img, 2 * ch_a), BF16),
                pltpu.VMEM((n_out_row + 2, w_out + 2, n_img, ch_b), BF16),
                pltpu.VMEM((n_row + 1, w_out * n_img, ch_b), F32),
                pltpu.VMEM((ch_b // 128, n_out_row * w_out * 17 + 7, 128), F32),
                pltpu.VMEM((n_out_row, n_img, w_out, ch_b), BF16),
                pltpu.VMEM((12 * ch_a, ch_b), BF16),
                pltpu.VMEM((9 * ch_a, ch_b), BF16),
                pltpu.VMEM((n_layers_b, 9 * ch_b, ch_b), BF16),
                pltpu.VMEM((n_stats, 2, ch_b), F32),
                pltpu.VMEM((n_stats, n_group, 2, ch_b), F32),
                dma((n_row,)), dma((28,)), dma((3,)), dma((3,)),
                dma((n_stats, n_group)), dma((n_stats, n_group)),
                dma((n_layers_b, 2)), dma((n_layers_b, 2)), dma((n_out_row,)),
            ],
            compiler_params=pltpu.CompilerParams(
                collective_id=0, has_side_effects=True, vmem_limit_bytes=67043328),
        )(img, w_a[0], norm_a, w_down, norm_down, w_b.reshape(n_layers_b, 9 * ch_b, ch_b), norm_b)

    act_spec = P(('pod', 'dp'), 'sp', None, None)
    return jax.shard_map(local_stack, mesh=mesh, in_specs=(act_spec, P(), P(), P(), P(), P(), P()), out_specs=act_spec, check_vma=False)
```

```python
import functools

import jax
import jax.numpy as jnp
from jax import lax
from jax.experimental import pallas as pl
from jax.experimental.pallas import tpu as pltpu
from jax.sharding import PartitionSpec as P

EPS_VALUE = 1e-5
MESH = pl.DeviceIdType.MESH
BF16 = jnp.bfloat16
F32 = jnp.float32


def stack_kernel(n_dp, n_sp, n_early, img, wa, na, wd, nd, wb, nb, out,
                 nat, stage, img_t, act_a, act_b, zbuf, zhalo, zfin, out_nat,
                 wa_v, wd_v, wb_v, stat_src, stat_dst,
                 in_sem, w_sem, halo_in_send, halo_in_recv, stat_send, stat_recv,
                 halo_send, halo_recv, early_send, early_recv, out_sem):
    n_img, n_row, width, ch_a = img.shape
    n_out_row, w_out, ch_b = out.shape[1], out.shape[2], out.shape[3]
    n_layers_b = wb.shape[0]
    n_group = n_dp * n_sp
    m_row = w_out * n_img
    my_pod, my_dp, my_sp = lax.axis_index("pod"), lax.axis_index("dp"), lax.axis_index("sp")
    me = my_dp * n_sp + my_sp
    is_top = my_sp == 0
    is_bottom = my_sp == n_sp - 1
    not_top = my_sp > 0
    not_bottom = my_sp < n_sp - 1
    upper = (my_pod, my_dp, lax.max(my_sp - 1, 0))
    lower = (my_pod, my_dp, lax.min(my_sp + 1, n_sp - 1))

    def peer(offset):
        flat = lax.rem(me + offset, n_group)
        return (my_pod, flat // n_sp, lax.rem(flat, n_sp))

    row_copies = [pltpu.make_async_copy(img.at[:, r], nat.at[r + 1], in_sem.at[r]) for r in range(n_row)]
    for c in row_copies:
        c.start()
    w_copies = []
    for p in range(3):
        for q in range(3):
            for half in range(2):
                k = q + half
                w_copies.append(pltpu.make_async_copy(
                    wa.at[p, q], wa_v.at[pl.ds(p * 4 * ch_a + k * ch_a, ch_a), pl.ds(half * ch_a, ch_a)],
                    w_sem.at[len(w_copies)]))
    for p in range(3):
        for q in range(3):
            off = p * 2 * ch_a + q * ch_a if q < 2 else 6 * ch_a + p * ch_a
            w_copies.append(pltpu.make_async_copy(wd.at[p, q], wd_v.at[pl.ds(off, ch_a)], w_sem.at[len(w_copies)]))
    w_copies.append(pltpu.make_async_copy(wb, wb_v, w_sem.at[len(w_copies)]))
    for c in w_copies:
        c.start()

    barrier = pltpu.get_barrier_semaphore()
    for i in range(1, n_group):
        pl.semaphore_signal(barrier, inc=1, device_id=peer(i), device_id_type=MESH)

    for p in range(3):
        wa_v[pl.ds(p * 4 * ch_a + 3 * ch_a, ch_a), 0:ch_a] = jnp.zeros((ch_a, ch_a), BF16)
        wa_v[pl.ds(p * 4 * ch_a, ch_a), ch_a:2 * ch_a] = jnp.zeros((ch_a, ch_a), BF16)
    n_rows_t = img_t.shape[0]
    img_t[:, 0, :, 0:ch_a] = jnp.zeros((n_rows_t, n_img, ch_a), BF16)
    img_t[:, w_out, :, ch_a:2 * ch_a] = jnp.zeros((n_rows_t, n_img, ch_a), BF16)
    act_a[:, w_out] = jnp.zeros((act_a.shape[0], n_img, 2 * ch_a), BF16)
    act_b[:, 0] = jnp.zeros((act_b.shape[0], n_img, ch_b), BF16)
    act_b[:, w_out + 1] = jnp.zeros((act_b.shape[0], n_img, ch_b), BF16)

    @pl.when(is_top)
    def _():
        nat[0] = jnp.zeros((n_img, width, ch_a), BF16)
        act_b[0] = jnp.zeros((w_out + 2, n_img, ch_b), BF16)

    @pl.when(is_bottom)
    def _():
        nat[n_row + 1] = jnp.zeros((n_img, width, ch_a), BF16)
        nat[n_row + 2] = jnp.zeros((n_img, width, ch_a), BF16)
        act_b[n_out_row + 1] = jnp.zeros((w_out + 2, n_img, ch_b), BF16)

    def image_halo(src_row, dst_row, dev, k):
        return pltpu.make_async_remote_copy(
            src_ref=img.at[:, src_row], dst_ref=nat.at[dst_row], send_sem=halo_in_send.at[k],
            recv_sem=halo_in_recv.at[k], device_id=dev, device_id_type=MESH)

    to_lower = image_halo(n_row - 1, 0, lower, 0)
    to_upper0 = image_halo(0, n_row + 1, upper, 1)
    to_upper1 = image_halo(1, n_row + 2, upper, 2)

    def transpose_row(k):
        pitch = stage.shape[0] // n_img

        for i in range(n_img):
            stage[pl.ds(i * pitch, width), :] = nat[k, i].astype(F32)
        for x in range(width):
            half = (x + 1) % 2
            img_t[k, (x + 1) // 2, :, half * ch_a:(half + 1) * ch_a] = (
                stage[pl.ds(x, n_img, stride=pitch), :].astype(BF16))

    def fold(total, z_val):
        z3 = z_val.reshape(m_row // 8, 8, ch_b)
        return total[0] + jnp.sum(z3, axis=0), total[1] + jnp.sum(z3 * z3, axis=0)

    def conv_a(r, rows=(0, 1, 2)):
        parts = []
        for p in rows:
            for k in range(2):
                parts.append(img_t[r + p, pl.ds(k, w_out)].reshape(m_row, 2 * ch_a))
        w_val = wa_v[pl.ds(rows[0] * 4 * ch_a, len(rows) * 4 * ch_a)]
        return jnp.dot(jnp.concatenate(parts, axis=1), w_val, preferred_element_type=F32)

    def conv_down(r):
        parts = [act_a[2 * r + p, pl.ds(0, w_out)].reshape(m_row, 2 * ch_a) for p in range(3)]
        parts += [act_a[2 * r + p, pl.ds(1, w_out), :, 0:ch_a].reshape(m_row, ch_a) for p in range(3)]
        return jnp.dot(jnp.concatenate(parts, axis=1), wd_v[...], preferred_element_type=F32)

    def conv_b(r, layer, rows=(0, 1, 2)):
        parts = []
        for p in rows:
            for q in range(3):
                parts.append(act_b[r + p, pl.ds(q, w_out)].reshape(m_row, ch_b))
        w_val = wb_v[layer, pl.ds(rows[0] * 3 * ch_b, len(rows) * 3 * ch_b)]
        return jnp.dot(jnp.concatenate(parts, axis=1), w_val, preferred_element_type=F32)

    def keep_z(r, z_val):
        zbuf[r] = z_val

    def keep_final(r, z_val):
        pitch = zfin.shape[1] // (n_out_row * w_out)
        for x in range(w_out):
            for h in range(ch_b // 128):
                zfin[h, pl.ds((r * w_out + x) * pitch, n_img), :] = z_val[x * n_img:(x + 1) * n_img, h * 128:(h + 1) * 128]

    def send_stats(layer, total):
        s1 = jnp.sum(total[0], axis=0, keepdims=True)
        s2 = jnp.sum(total[1], axis=0, keepdims=True)
        if layer == 0:
            s1 = s1[:, :ch_a] + s1[:, ch_a:]
            s2 = s2[:, :ch_a] + s2[:, ch_a:]
            s1 = jnp.concatenate([s1, s1], axis=1)
            s2 = jnp.concatenate([s2, s2], axis=1)
        both = jnp.concatenate([s1, s2], axis=0)
        stat_src[layer] = both
        stat_dst[layer, me] = both
        copies = []
        for i in range(1, n_group):
            copies.append(pltpu.make_async_remote_copy(
                src_ref=stat_src.at[layer], dst_ref=stat_dst.at[layer, me], send_sem=stat_send.at[layer, i],
                recv_sem=stat_recv.at[layer, i], device_id=peer(i), device_id_type=MESH))
        for c in copies:
            c.start()
        return copies

    def finish_stats(layer, copies, gamma, beta, count):
        with jax.named_scope("stats_wait"):
            for c in copies:
                c.wait()
        tot = jnp.sum(stat_dst[layer], axis=0)
        mean = tot[0:1] / count
        var = tot[1:2] / count - mean * mean
        scale = gamma * lax.rsqrt(var + EPS_VALUE)
        return mean, scale, beta

    def normalize(z_val, coef):
        mean, scale, beta = coef
        return jnp.maximum((z_val - mean) * scale + beta, 0.0).astype(BF16)

    zeros = (jnp.zeros((8, ch_b), F32), jnp.zeros((8, ch_b), F32))

    def t_body(r, carry):
        pltpu.make_async_copy(img.at[:, r], nat.at[r + 1], in_sem.at[r]).wait()
        transpose_row(r + 1)
        return carry

    with jax.named_scope("transpose"):
        lax.fori_loop(0, n_row, t_body, 0)
    with jax.named_scope("barrier"):
        pl.semaphore_wait(barrier, n_group - 1)

    @pl.when(not_bottom)
    def _():
        to_lower.start()

    @pl.when(not_top)
    def _():
        to_upper0.start()
        to_upper1.start()

    for c in w_copies:
        c.wait()

    def a_body(i, total):
        r = 1 + 2 * i
        z_pair = [conv_a(r), conv_a(r + 1)]
        for j in range(2):
            keep_z(r + j, z_pair[j])
            total = fold(total, z_pair[j])
        return total

    with jax.named_scope("conv_a"):
        total = lax.fori_loop(0, (n_row - 2) // 2, a_body, zeros)
    with jax.named_scope("conv_a_part"):
        keep_z(0, conv_a(0, (1, 2)))
        keep_z(n_row - 1, conv_a(n_row - 1, (0, 1)))
    with jax.named_scope("img_halo_wait"):
        @pl.when(not_top)
        def _():
            to_lower.wait_recv()

        @pl.when(not_bottom)
        def _():
            to_upper0.wait_recv()

    with jax.named_scope("transpose_halo"):
        transpose_row(0)
        transpose_row(n_row + 1)
    with jax.named_scope("conv_a_edge"):
        for r, p in ((0, 0), (n_row - 1, 2)):
            z_val = conv_a(r, (p,)) + zbuf[r]
            keep_z(r, z_val)
            total = fold(total, z_val)
    with jax.named_scope("send_stats"):
        copies = send_stats(0, total)
    with jax.named_scope("img_halo_wait2"):
        @pl.when(not_bottom)
        def _():
            to_upper1.wait_recv()

    with jax.named_scope("conv_a_extra"):
        transpose_row(n_row + 2)
        zbuf[n_row] = conv_a(n_row)
    n_a = float(n_group * n_img * n_row * width)
    wide = lambda v: jnp.concatenate([v, v], axis=1)
    coef_a = finish_stats(0, copies, wide(na[0, 0:1]), wide(na[0, 1:2]), n_a)

    def norm_a_row(r):
        y_val = normalize(zbuf[r], coef_a)
        if r == n_row:
            y_val = jnp.where(is_bottom, jnp.zeros_like(y_val), y_val)
        act_a[r, pl.ds(0, w_out)] = y_val.reshape(w_out, n_img, 2 * ch_a)

    with jax.named_scope("conv_down"):
        total = zeros
        norm_a_row(0)
        for r in range(n_out_row):
            norm_a_row(2 * r + 1)
            norm_a_row(2 * r + 2)
            z_val = conv_down(r)
            zbuf[2 * r] = z_val
            total = fold(total, z_val)

    n_late = w_out - n_early
    last_row = n_out_row - 1

    def z_row(layer, r):
        return 2 * r if layer == 0 else r

    def early_copies(layer):
        slot = layer % 2
        up = pltpu.make_async_remote_copy(
            src_ref=zbuf.at[z_row(layer, 0), pl.ds(0, n_early * n_img)], dst_ref=zhalo.at[slot, 1], send_sem=early_send.at[layer, 1],
            recv_sem=early_recv.at[layer, 1], device_id=upper, device_id_type=MESH)
        down = pltpu.make_async_remote_copy(
            src_ref=zbuf.at[z_row(layer, last_row), pl.ds(0, n_early * n_img)], dst_ref=zhalo.at[slot, 0], send_sem=early_send.at[layer, 0],
            recv_sem=early_recv.at[layer, 0], device_id=lower, device_id_type=MESH)
        return up, down

    def late_copies(layer):
        cols = pl.ds(1 + n_early, n_late)
        up = pltpu.make_async_remote_copy(
            src_ref=act_b.at[1, cols], dst_ref=act_b.at[n_out_row + 1, cols],
            send_sem=halo_send.at[layer, 1], recv_sem=halo_recv.at[layer, 1], device_id=upper, device_id_type=MESH)
        down = pltpu.make_async_remote_copy(
            src_ref=act_b.at[n_out_row, cols], dst_ref=act_b.at[0, cols],
            send_sem=halo_send.at[layer, 0], recv_sem=halo_recv.at[layer, 0], device_id=lower, device_id_type=MESH)
        return up, down

    def start_both(up, down):
        @pl.when(not_top)
        def _():
            up.start()

        @pl.when(not_bottom)
        def _():
            down.start()

    n_b = float(n_group * m_row * n_out_row)
    with jax.named_scope("send_stats"):
        copies = send_stats(1, total)
        up_early, down_early = early_copies(0)
        start_both(up_early, down_early)
    coef = finish_stats(1, copies, nd[0:1], nd[1:2], n_b)

    for layer in range(n_layers_b):
        def norm_b_cols(r, first, count):
            z_val = zbuf[z_row(layer, r), pl.ds(first * n_img, count * n_img)]
            act_b[r + 1, pl.ds(1 + first, count)] = normalize(z_val, coef).reshape(count, n_img, ch_b)

        up, down = late_copies(layer)
        with jax.named_scope("norm_edge"):
            norm_b_cols(0, n_early, n_late)
            norm_b_cols(last_row, n_early, n_late)
            start_both(up, down)

        last = layer == n_layers_b - 1
        keep = keep_final if last else keep_z
        with jax.named_scope("conv_b_main"):
            norm_b_cols(0, 0, n_early)
            norm_b_cols(last_row, 0, n_early)
            for r in range(1, last_row):
                norm_b_cols(r, 0, w_out)
            total = zeros
            zbuf[n_row - 1] = conv_b(0, layer, (1, 2))
            for r in range(1, last_row):
                z_val = conv_b(r, layer)
                keep(r, z_val)
                total = fold(total, z_val)
            zbuf[n_row] = conv_b(last_row, layer, (0, 1))

        with jax.named_scope("halo_wait"):
            def norm_halo(side, row):
                y_val = normalize(zhalo[layer % 2, side], coef)
                act_b[row, pl.ds(1, n_early)] = y_val.reshape(n_early, n_img, ch_b)

            @pl.when(not_top)
            def _():
                up_early.wait_send()
                down_early.wait_recv()
                norm_halo(0, 0)
                up.wait_send()
                down.wait_recv()

            @pl.when(not_bottom)
            def _():
                down_early.wait_send()
                up_early.wait_recv()
                norm_halo(1, n_out_row + 1)
                down.wait_send()
                up.wait_recv()

        with jax.named_scope("conv_b_edge"):
            for j, r, p in ((0, 0, 0), (1, last_row, 2)):
                z_val = conv_b(r, layer, (p,)) + zbuf[n_row - 1 + j]
                keep(r, z_val)
                total = fold(total, z_val)

        with jax.named_scope("send_stats"):
            copies = send_stats(2 + layer, total)
            if not last:
                up_early, down_early = early_copies(layer + 1)
                start_both(up_early, down_early)
        coef = finish_stats(2 + layer, copies, nb[layer, 0:1], nb[layer, 1:2], n_b)

    pitch = zfin.shape[1] // (n_out_row * w_out)

    def out_body(r, carry):
        for i in range(n_img):
            for h in range(ch_b // 128):
                lanes = slice(h * 128, (h + 1) * 128)
                z_val = zfin[h, pl.ds(r * w_out * pitch + i, w_out, stride=pitch), :]
                out_nat[r, i, :, lanes] = normalize(z_val, tuple(v[:, lanes] for v in coef))
        pltpu.make_async_copy(out_nat.at[r], out.at[:, r], out_sem.at[r]).start()
        return carry

    with jax.named_scope("final_norm"):
        lax.fori_loop(0, n_out_row, out_body, 0)
    for r in range(n_out_row):
        pltpu.make_async_copy(out_nat.at[r], out.at[:, r], out_sem.at[r]).wait()

    @pl.when(not_bottom)
    def _():
        to_lower.wait_send()

    @pl.when(not_top)
    def _():
        to_upper0.wait_send()
        to_upper1.wait_send()


def solution(mesh):
    n_sp, n_dp = mesh.shape['sp'], mesh.shape['dp']

    def local_stack(img, w_a, norm_a, w_down, norm_down, w_b, norm_b):
        n_img, n_row, width, ch_a = img.shape
        ch_b = w_down.shape[-1]
        n_out_row, w_out = n_row // 2, width // 2
        n_layers_b = w_b.shape[0]
        n_group = n_sp * n_dp
        any_spec = pl.BlockSpec(memory_space=pl.ANY)
        vmem_spec = pl.BlockSpec(memory_space=pltpu.VMEM)
        dma = pltpu.SemaphoreType.DMA
        n_stats = 2 + n_layers_b
        n_early = w_out // 3
        return pl.pallas_call(
            functools.partial(stack_kernel, n_dp, n_sp, n_early),
            out_shape=jax.ShapeDtypeStruct((n_img, n_out_row, w_out, ch_b), BF16),
            in_specs=[any_spec, any_spec, vmem_spec, any_spec, vmem_spec, any_spec, vmem_spec],
            out_specs=any_spec,
            scratch_shapes=[
                pltpu.VMEM((n_row + 3, n_img, width, ch_a), BF16),
                pltpu.VMEM((n_img * width, 128), F32),
                pltpu.VMEM((n_row + 3, w_out + 1, n_img, 2 * ch_a), BF16),
                pltpu.VMEM((n_row + 1, w_out + 1, n_img, 2 * ch_a), BF16),
                pltpu.VMEM((n_out_row + 2, w_out + 2, n_img, ch_b), BF16),
                pltpu.VMEM((n_row + 1, w_out * n_img, ch_b), F32),
                pltpu.VMEM((2, 2, n_early * n_img, ch_b), F32),
                pltpu.VMEM((ch_b // 128, n_out_row * w_out * 17 + 7, 128), F32),
                pltpu.VMEM((n_out_row, n_img, w_out, ch_b), BF16),
                pltpu.VMEM((12 * ch_a, ch_b), BF16),
                pltpu.VMEM((9 * ch_a, ch_b), BF16),
                pltpu.VMEM((n_layers_b, 9 * ch_b, ch_b), BF16),
                pltpu.VMEM((n_stats, 2, ch_b), F32),
                pltpu.VMEM((n_stats, n_group, 2, ch_b), F32),
                dma((n_row,)), dma((28,)), dma((3,)), dma((3,)),
                dma((n_stats, n_group)), dma((n_stats, n_group)),
                dma((n_layers_b, 2)), dma((n_layers_b, 2)), dma((n_layers_b, 2)), dma((n_layers_b, 2)), dma((n_out_row,)),
            ],
            compiler_params=pltpu.CompilerParams(
                collective_id=0, has_side_effects=True, vmem_limit_bytes=67043328),
        )(img, w_a[0], norm_a, w_down, norm_down, w_b.reshape(n_layers_b, 9 * ch_b, ch_b), norm_b)

    act_spec = P(('pod', 'dp'), 'sp', None, None)
    return jax.shard_map(local_stack, mesh=mesh, in_specs=(act_spec, P(), P(), P(), P(), P(), P()), out_specs=act_spec, check_vma=False)
```

```python
import functools

import jax
import jax.numpy as jnp
from jax import lax
from jax.experimental import pallas as pl
from jax.experimental.pallas import tpu as pltpu
from jax.sharding import PartitionSpec as P

EPS_VALUE = 1e-5
MESH = pl.DeviceIdType.MESH
BF16 = jnp.bfloat16
F32 = jnp.float32


def stack_kernel(n_dp, n_sp, n_early, img, wa, na, wd, nd, wb, nb, z_out, stat_out,
                 nat, stage, img_t, act_a, act_b, zbuf, zhalo, zfin,
                 wa_v, wd_v, wb_v, stat_src, stat_dst,
                 in_sem, w_sem, halo_in_send, halo_in_recv, stat_send, stat_recv,
                 halo_send, halo_recv, early_send, early_recv, out_sem, own_sem):
    n_img, n_row, width, ch_a = img.shape
    n_out_row, w_out, ch_b = n_row // 2, width // 2, wd.shape[3]
    n_layers_b = wb.shape[0]
    n_group = n_dp * n_sp
    m_row = w_out * n_img
    my_pod, my_dp, my_sp = lax.axis_index("pod"), lax.axis_index("dp"), lax.axis_index("sp")
    me = my_dp * n_sp + my_sp
    is_top = my_sp == 0
    is_bottom = my_sp == n_sp - 1
    not_top = my_sp > 0
    not_bottom = my_sp < n_sp - 1
    upper = (my_pod, my_dp, lax.max(my_sp - 1, 0))
    lower = (my_pod, my_dp, lax.min(my_sp + 1, n_sp - 1))

    def peer(offset):
        flat = lax.rem(me + offset, n_group)
        return (my_pod, flat // n_sp, lax.rem(flat, n_sp))

    row_copies = [pltpu.make_async_copy(img.at[:, r], nat.at[r + 1], in_sem.at[r]) for r in range(n_row)]
    for c in row_copies:
        c.start()
    w_copies = []
    for p in range(3):
        for q in range(3):
            for half in range(2):
                k = q + half
                w_copies.append(pltpu.make_async_copy(
                    wa.at[p, q], wa_v.at[pl.ds(p * 4 * ch_a + k * ch_a, ch_a), pl.ds(half * ch_a, ch_a)],
                    w_sem.at[len(w_copies)]))
    for p in range(3):
        for q in range(3):
            off = p * 2 * ch_a + q * ch_a if q < 2 else 6 * ch_a + p * ch_a
            w_copies.append(pltpu.make_async_copy(wd.at[p, q], wd_v.at[pl.ds(off, ch_a)], w_sem.at[len(w_copies)]))
    w_copies.append(pltpu.make_async_copy(wb, wb_v, w_sem.at[len(w_copies)]))
    for c in w_copies:
        c.start()

    barrier = pltpu.get_barrier_semaphore()
    for i in range(1, n_group):
        pl.semaphore_signal(barrier, inc=1, device_id=peer(i), device_id_type=MESH)

    for p in range(3):
        wa_v[pl.ds(p * 4 * ch_a + 3 * ch_a, ch_a), 0:ch_a] = jnp.zeros((ch_a, ch_a), BF16)
        wa_v[pl.ds(p * 4 * ch_a, ch_a), ch_a:2 * ch_a] = jnp.zeros((ch_a, ch_a), BF16)
    n_rows_t = img_t.shape[0]
    img_t[:, 0, :, 0:ch_a] = jnp.zeros((n_rows_t, n_img, ch_a), BF16)
    img_t[:, w_out, :, ch_a:2 * ch_a] = jnp.zeros((n_rows_t, n_img, ch_a), BF16)
    act_a[:, w_out] = jnp.zeros((act_a.shape[0], n_img, 2 * ch_a), BF16)
    act_b[:, 0] = jnp.zeros((act_b.shape[0], n_img, ch_b), BF16)
    act_b[:, w_out + 1] = jnp.zeros((act_b.shape[0], n_img, ch_b), BF16)

    @pl.when(is_top)
    def _():
        nat[0] = jnp.zeros((n_img, width, ch_a), BF16)
        act_b[0] = jnp.zeros((w_out + 2, n_img, ch_b), BF16)

    @pl.when(is_bottom)
    def _():
        nat[n_row + 1] = jnp.zeros((n_img, width, ch_a), BF16)
        nat[n_row + 2] = jnp.zeros((n_img, width, ch_a), BF16)
        act_b[n_out_row + 1] = jnp.zeros((w_out + 2, n_img, ch_b), BF16)

    def image_halo(src_row, dst_row, dev, k):
        return pltpu.make_async_remote_copy(
            src_ref=img.at[:, src_row], dst_ref=nat.at[dst_row], send_sem=halo_in_send.at[k],
            recv_sem=halo_in_recv.at[k], device_id=dev, device_id_type=MESH)

    to_lower = image_halo(n_row - 1, 0, lower, 0)
    to_upper0 = image_halo(0, n_row + 1, upper, 1)
    cols_x = width * 4 // 7 // 16 * 16
    n_pair = cols_x // 2 - 1
    to_upper1 = pltpu.make_async_remote_copy(
        src_ref=img.at[:, 1, pl.ds(0, cols_x)], dst_ref=nat.at[n_row + 2, :, pl.ds(0, cols_x)], send_sem=halo_in_send.at[2],
        recv_sem=halo_in_recv.at[2], device_id=upper, device_id_type=MESH)
    far = pl.ds(n_pair * n_img, (w_out - n_pair) * n_img)
    to_upper_z = pltpu.make_async_remote_copy(
        src_ref=zbuf.at[0, far], dst_ref=zbuf.at[n_row, far], send_sem=halo_in_send.at[3],
        recv_sem=halo_in_recv.at[3], device_id=upper, device_id_type=MESH)

    def transpose_row(k, cols=width):
        pitch = stage.shape[0] // n_img

        for i in range(n_img):
            stage[pl.ds(i * pitch, cols), :] = nat[k, i, 0:cols].astype(F32)
        for x in range(cols):
            half = (x + 1) % 2
            img_t[k, (x + 1) // 2, :, half * ch_a:(half + 1) * ch_a] = (
                stage[pl.ds(x, n_img, stride=pitch), :].astype(BF16))

    def fold(total, z_val):
        z3 = z_val.reshape(m_row // 8, 8, ch_b)
        return total[0] + jnp.sum(z3, axis=0), total[1] + jnp.sum(z3 * z3, axis=0)

    def conv_a(r, rows=(0, 1, 2), pairs=w_out):
        parts = []
        for p in rows:
            for k in range(2):
                parts.append(img_t[r + p, pl.ds(k, pairs)].reshape(pairs * n_img, 2 * ch_a))
        w_val = wa_v[pl.ds(rows[0] * 4 * ch_a, len(rows) * 4 * ch_a)]
        return jnp.dot(jnp.concatenate(parts, axis=1), w_val, preferred_element_type=F32)

    def conv_down(r):
        parts = [act_a[2 * r + p, pl.ds(0, w_out)].reshape(m_row, 2 * ch_a) for p in range(3)]
        parts += [act_a[2 * r + p, pl.ds(1, w_out), :, 0:ch_a].reshape(m_row, ch_a) for p in range(3)]
        return jnp.dot(jnp.concatenate(parts, axis=1), wd_v[...], preferred_element_type=F32)

    def conv_b(r, layer, rows=(0, 1, 2)):
        parts = []
        for p in rows:
            for q in range(3):
                parts.append(act_b[r + p, pl.ds(q, w_out)].reshape(m_row, ch_b))
        w_val = wb_v[layer, pl.ds(rows[0] * 3 * ch_b, len(rows) * 3 * ch_b)]
        return jnp.dot(jnp.concatenate(parts, axis=1), w_val, preferred_element_type=F32)

    def keep_z(r, z_val):
        zbuf[r] = z_val

    def keep_final(r, z_val):
        for x in range(w_out):
            for h in range(ch_b // 128):
                zfin[h, pl.ds(x * n_img * n_out_row + r, n_img, stride=n_out_row), :] = (
                    z_val[x * n_img:(x + 1) * n_img, h * 128:(h + 1) * 128])

    def send_stats(layer, total):
        s1 = jnp.sum(total[0], axis=0, keepdims=True)
        s2 = jnp.sum(total[1], axis=0, keepdims=True)
        if layer == 0:
            s1 = s1[:, :ch_a] + s1[:, ch_a:]
            s2 = s2[:, :ch_a] + s2[:, ch_a:]
            s1 = jnp.concatenate([s1, s1], axis=1)
            s2 = jnp.concatenate([s2, s2], axis=1)
        both = jnp.concatenate([s1, s2], axis=0)
        stat_src[layer] = both
        last = layer == stat_src.shape[0] - 1
        slot = stat_out.at[me] if last else stat_dst.at[layer, me]
        if not last:
            stat_dst[layer, me] = both
        copies = []
        for i in range(1, n_group):
            copies.append(pltpu.make_async_remote_copy(
                src_ref=stat_src.at[layer], dst_ref=slot, send_sem=stat_send.at[layer, i],
                recv_sem=stat_recv.at[layer, i], device_id=peer(i), device_id_type=MESH))
        for c in copies:
            c.start()
        if last:
            copies.append(pltpu.make_async_copy(stat_src.at[layer], slot, own_sem))
            copies[-1].start()
        return copies

    def finish_stats(layer, copies, gamma, beta, count):
        with jax.named_scope("stats_wait"):
            for c in copies:
                c.wait()
        tot = jnp.sum(stat_dst[layer], axis=0)
        mean = tot[0:1] / count
        var = tot[1:2] / count - mean * mean
        scale = gamma * lax.rsqrt(var + EPS_VALUE)
        return scale, beta - mean * scale

    def normalize(z_val, coef):
        scale, shift = coef
        return jnp.maximum(z_val * scale + shift, 0.0).astype(BF16)

    def z_row(layer, r):
        return 2 * r + (layer + 1) % 2

    zeros = (jnp.zeros((8, ch_b), F32), jnp.zeros((8, ch_b), F32))

    def t_body(r, carry):
        pltpu.make_async_copy(img.at[:, r], nat.at[r + 1], in_sem.at[r]).wait()
        transpose_row(r + 1)
        return carry

    with jax.named_scope("transpose"):
        lax.fori_loop(0, n_row, t_body, 0)
    with jax.named_scope("barrier"):
        pl.semaphore_wait(barrier, n_group - 1)

    @pl.when(not_bottom)
    def _():
        to_lower.start()

    @pl.when(not_top)
    def _():
        to_upper0.start()
        to_upper1.start()

    for c in w_copies:
        c.wait()

    def a_body(i, total):
        r = 1 + 2 * i
        z_pair = [conv_a(r), conv_a(r + 1)]
        for j in range(2):
            keep_z(r + j, z_pair[j])
            total = fold(total, z_pair[j])
        return total

    with jax.named_scope("conv_a"):
        total = lax.fori_loop(0, (n_row - 2) // 2, a_body, zeros)
    with jax.named_scope("conv_a_part"):
        keep_z(0, conv_a(0, (1, 2)))
        keep_z(n_row - 1, conv_a(n_row - 1, (0, 1)))
    with jax.named_scope("img_halo_wait"):
        @pl.when(not_top)
        def _():
            to_lower.wait_recv()

        @pl.when(not_bottom)
        def _():
            to_upper0.wait_recv()

    with jax.named_scope("transpose_halo"):
        transpose_row(0)
        transpose_row(n_row + 1)
    with jax.named_scope("conv_a_edge"):
        for r, p in ((0, 0), (n_row - 1, 2)):
            z_val = conv_a(r, (p,)) + zbuf[r]
            keep_z(r, z_val)
            total = fold(total, z_val)
    with jax.named_scope("send_stats"):
        copies = send_stats(0, total)

        @pl.when(not_top)
        def _():
            to_upper_z.start()

    with jax.named_scope("img_halo_wait2"):
        @pl.when(not_bottom)
        def _():
            to_upper1.wait_recv()

    with jax.named_scope("conv_a_extra"):
        transpose_row(n_row + 2, cols_x)
        zbuf[n_row, 0:n_pair * n_img] = conv_a(n_row, pairs=n_pair)
    n_a = float(n_group * n_img * n_row * width)
    wide = lambda v: jnp.concatenate([v, v], axis=1)
    coef_a = finish_stats(0, copies, wide(na[0, 0:1]), wide(na[0, 1:2]), n_a)

    def norm_a_row(r):
        y_val = normalize(zbuf[r], coef_a)
        if r == n_row:
            y_val = jnp.where(is_bottom, jnp.zeros_like(y_val), y_val)
        act_a[r, pl.ds(0, w_out)] = y_val.reshape(w_out, n_img, 2 * ch_a)

    def down_row(r, total):
        z_val = conv_down(r)
        zbuf[z_row(0, r)] = z_val
        return fold(total, z_val)

    with jax.named_scope("conv_down"):
        total = zeros
        norm_a_row(0)
        for r in range(n_out_row - 1):
            norm_a_row(2 * r + 1)
            norm_a_row(2 * r + 2)
            total = down_row(r, total)
        norm_a_row(n_row - 1)
    with jax.named_scope("down_halo_wait"):
        @pl.when(not_top)
        def _():
            to_upper_z.wait_send()

        @pl.when(not_bottom)
        def _():
            to_upper_z.wait_recv()

    with jax.named_scope("conv_down_last"):
        norm_a_row(n_row)
        total = down_row(n_out_row - 1, total)

    n_late = w_out - n_early
    last_row = n_out_row - 1

    def early_copies(layer):
        slot = layer % 2
        up = pltpu.make_async_remote_copy(
            src_ref=zbuf.at[z_row(layer, 0), pl.ds(0, n_early * n_img)], dst_ref=zhalo.at[slot, 1], send_sem=early_send.at[layer, 1],
            recv_sem=early_recv.at[layer, 1], device_id=upper, device_id_type=MESH)
        down = pltpu.make_async_remote_copy(
            src_ref=zbuf.at[z_row(layer, last_row), pl.ds(0, n_early * n_img)], dst_ref=zhalo.at[slot, 0], send_sem=early_send.at[layer, 0],
            recv_sem=early_recv.at[layer, 0], device_id=lower, device_id_type=MESH)
        return up, down

    def late_copies(layer):
        cols = pl.ds(1 + n_early, n_late)
        up = pltpu.make_async_remote_copy(
            src_ref=act_b.at[1, cols], dst_ref=act_b.at[n_out_row + 1, cols],
            send_sem=halo_send.at[layer, 1], recv_sem=halo_recv.at[layer, 1], device_id=upper, device_id_type=MESH)
        down = pltpu.make_async_remote_copy(
            src_ref=act_b.at[n_out_row, cols], dst_ref=act_b.at[0, cols],
            send_sem=halo_send.at[layer, 0], recv_sem=halo_recv.at[layer, 0], device_id=lower, device_id_type=MESH)
        return up, down

    def start_both(up, down):
        @pl.when(not_top)
        def _():
            up.start()

        @pl.when(not_bottom)
        def _():
            down.start()

    n_b = float(n_group * m_row * n_out_row)
    with jax.named_scope("send_stats"):
        copies = send_stats(1, total)
        up_early, down_early = early_copies(0)
        start_both(up_early, down_early)
    coef = finish_stats(1, copies, nd[0:1], nd[1:2], n_b)

    for layer in range(n_layers_b):
        def norm_b_cols(r, first, count):
            z_val = zbuf[z_row(layer, r), pl.ds(first * n_img, count * n_img)]
            act_b[r + 1, pl.ds(1 + first, count)] = normalize(z_val, coef).reshape(count, n_img, ch_b)

        up, down = late_copies(layer)
        with jax.named_scope("norm_edge"):
            norm_b_cols(0, n_early, n_late)
            norm_b_cols(last_row, n_early, n_late)
            start_both(up, down)

        last = layer == n_layers_b - 1
        def keep(r, z_val):
            if last:
                keep_final(r, z_val)
            else:
                zbuf[z_row(layer + 1, r)] = z_val

        with jax.named_scope("conv_b_main"):
            norm_b_cols(0, 0, n_early)
            norm_b_cols(last_row, 0, n_early)
            for r in range(1, last_row):
                norm_b_cols(r, 0, w_out)
            total = zeros
            zbuf[z_row(layer + 1, 0)] = conv_b(0, layer, (1, 2))
            for r in range(1, last_row):
                z_val = conv_b(r, layer)
                keep(r, z_val)
                total = fold(total, z_val)
            zbuf[z_row(layer + 1, last_row)] = conv_b(last_row, layer, (0, 1))

        with jax.named_scope("halo_wait"):
            def norm_halo(side, row):
                y_val = normalize(zhalo[layer % 2, side], coef)
                act_b[row, pl.ds(1, n_early)] = y_val.reshape(n_early, n_img, ch_b)

            @pl.when(not_top)
            def _():
                up_early.wait_send()
                down_early.wait_recv()
                norm_halo(0, 0)
                up.wait_send()
                down.wait_recv()

            @pl.when(not_bottom)
            def _():
                down_early.wait_send()
                up_early.wait_recv()
                norm_halo(1, n_out_row + 1)
                down.wait_send()
                up.wait_recv()

        with jax.named_scope("conv_b_edge"):
            for r, p in ((0, 0), (last_row, 2)):
                z_val = conv_b(r, layer, (p,)) + zbuf[z_row(layer + 1, r)]
                keep(r, z_val)
                total = fold(total, z_val)

        with jax.named_scope("send_stats"):
            copies = send_stats(2 + layer, total)
            if not last:
                up_early, down_early = early_copies(layer + 1)
                start_both(up_early, down_early)
        if not last:
            coef = finish_stats(2 + layer, copies, nb[layer, 0:1], nb[layer, 1:2], n_b)

    with jax.named_scope("z_out"):
        z_copy = pltpu.make_async_copy(zfin, z_out, out_sem)
        z_copy.start()
        z_copy.wait()
    with jax.named_scope("last_stats_wait"):
        for c in copies:
            c.wait()

    @pl.when(not_bottom)
    def _():
        to_lower.wait_send()

    @pl.when(not_top)
    def _():
        to_upper0.wait_send()
        to_upper1.wait_send()


def finish_kernel(count, z_hbm, stat_hbm, norm_hbm, out, z_v, stat, norms, out_v, z_sem, small_sem, out_sem):
    n_img, w_out, n_out_row, ch_b = out.shape
    n_chunk = z_sem.shape[0]
    chunk = w_out // n_chunk
    per_col = n_img * n_out_row

    def z_copy(k):
        rows = pl.ds(k * chunk * per_col, chunk * per_col)
        return pltpu.make_async_copy(z_hbm.at[:, rows], z_v.at[:, rows], z_sem.at[k])

    def out_copies(k):
        cols = pl.ds(k * chunk, chunk)
        return [pltpu.make_async_copy(out_v.at[cols, i], out.at[i, cols], out_sem.at[i, k]) for i in range(n_img)]

    small = [pltpu.make_async_copy(stat_hbm, stat, small_sem.at[0]), pltpu.make_async_copy(norm_hbm, norms, small_sem.at[1])]
    for c in small:
        c.start()
    for k in range(n_chunk):
        z_copy(k).start()
    for c in small:
        c.wait()
    norm = norms[norms.shape[0] - 1]
    tot = jnp.sum(stat[...], axis=0)
    mean = tot[0:1] / count
    var = tot[1:2] / count - mean * mean
    scale = norm[0:1] * lax.rsqrt(var + EPS_VALUE)
    shift = norm[1:2] - mean * scale
    for k in range(n_chunk):
        z_copy(k).wait()

        def out_body(x, carry):
            for h in range(ch_b // 128):
                lanes = slice(h * 128, (h + 1) * 128)
                z_val = z_v[h, pl.ds(x * per_col, per_col), :]
                y_val = jnp.maximum(z_val * scale[:, lanes] + shift[:, lanes], 0.0).astype(BF16)
                out_v[x, :, :, lanes] = y_val.reshape(n_img, n_out_row, 128)
            return carry

        lax.fori_loop(k * chunk, (k + 1) * chunk, out_body, 0, unroll=3)
        for c in out_copies(k):
            c.start()
    for k in range(n_chunk):
        for c in out_copies(k):
            c.wait()


def solution(mesh):
    n_sp, n_dp = mesh.shape['sp'], mesh.shape['dp']

    def local_stack(img, w_a, norm_a, w_down, norm_down, w_b, norm_b):
        n_img, n_row, width, ch_a = img.shape
        ch_b = w_down.shape[-1]
        n_out_row, w_out = n_row // 2, width // 2
        n_layers_b = w_b.shape[0]
        n_group = n_sp * n_dp
        any_spec = pl.BlockSpec(memory_space=pl.ANY)
        vmem_spec = pl.BlockSpec(memory_space=pltpu.VMEM)
        dma = pltpu.SemaphoreType.DMA
        n_stats = 2 + n_layers_b
        n_early = w_out // 3
        z_val, stats = pl.pallas_call(
            functools.partial(stack_kernel, n_dp, n_sp, n_early),
            out_shape=(
                jax.ShapeDtypeStruct((ch_b // 128, n_out_row * w_out * n_img, 128), F32),
                jax.ShapeDtypeStruct((n_group, 2, ch_b), F32),
            ),
            in_specs=[any_spec, any_spec, vmem_spec, any_spec, vmem_spec, any_spec, vmem_spec],
            out_specs=(any_spec, any_spec),
            scratch_shapes=[
                pltpu.VMEM((n_row + 3, n_img, width, ch_a), BF16),
                pltpu.VMEM((n_img * width, 128), F32),
                pltpu.VMEM((n_row + 3, w_out + 1, n_img, 2 * ch_a), BF16),
                pltpu.VMEM((n_row + 1, w_out + 1, n_img, 2 * ch_a), BF16),
                pltpu.VMEM((n_out_row + 2, w_out + 2, n_img, ch_b), BF16),
                pltpu.VMEM((n_row + 1, w_out * n_img, ch_b), F32),
                pltpu.VMEM((2, 2, n_early * n_img, ch_b), F32),
                pltpu.VMEM((ch_b // 128, n_out_row * w_out * n_img, 128), F32),
                pltpu.VMEM((12 * ch_a, ch_b), BF16),
                pltpu.VMEM((9 * ch_a, ch_b), BF16),
                pltpu.VMEM((n_layers_b, 9 * ch_b, ch_b), BF16),
                pltpu.VMEM((n_stats, 2, ch_b), F32),
                pltpu.VMEM((n_stats - 1, n_group, 2, ch_b), F32),
                dma((n_row,)), dma((28,)), dma((4,)), dma((4,)),
                dma((n_stats, n_group)), dma((n_stats, n_group)),
                dma((n_layers_b, 2)), dma((n_layers_b, 2)), dma((n_layers_b, 2)), dma((n_layers_b, 2)), dma, dma,
            ],
            compiler_params=pltpu.CompilerParams(
                collective_id=0, has_side_effects=True, vmem_limit_bytes=67043328),
        )(img, w_a[0], norm_a, w_down, norm_down, w_b.reshape(n_layers_b, 9 * ch_b, ch_b), norm_b)
        features = pl.pallas_call(
            functools.partial(finish_kernel, float(n_group * n_img * n_out_row * w_out)),
            out_shape=jax.ShapeDtypeStruct((n_img, w_out, n_out_row, ch_b), BF16),
            in_specs=[any_spec, any_spec, any_spec],
            out_specs=any_spec,
            scratch_shapes=[
                pltpu.VMEM(z_val.shape, F32),
                pltpu.VMEM(stats.shape, F32),
                pltpu.VMEM(norm_b.shape, F32),
                pltpu.VMEM((w_out, n_img, n_out_row, ch_b), BF16),
                dma((4,)), dma((2,)), dma((n_img, 4)),
            ],
            compiler_params=pltpu.CompilerParams(vmem_limit_bytes=67043328),
        )(z_val, stats, norm_b)
        return features.transpose(0, 2, 1, 3)

    act_spec = P(('pod', 'dp'), 'sp', None, None)
    return jax.shard_map(local_stack, mesh=mesh, in_specs=(act_spec, P(), P(), P(), P(), P(), P()), out_specs=act_spec, check_vma=False)
```

```python
import functools

import jax
import jax.numpy as jnp
from jax import lax
from jax.experimental import pallas as pl
from jax.experimental.pallas import tpu as pltpu
from jax.sharding import PartitionSpec as P

EPS_VALUE = 1e-5
MESH = pl.DeviceIdType.MESH
BF16 = jnp.bfloat16
F32 = jnp.float32


def stack_kernel(n_dp, n_sp, n_early, img, wa, na, wd, nd, wb, nb, z_out, stat_out,
                 nat, stage, img_t, act_a, act_b, zbuf, zhalo, zfin,
                 wa_v, wd_v, wb_v, stat_src, stat_dst,
                 in_sem, w_sem, halo_in_send, halo_in_recv, stat_send, stat_recv,
                 halo_send, halo_recv, early_send, early_recv, out_sem, own_sem):
    n_img, n_row, width, ch_a = img.shape
    n_out_row, w_out, ch_b = n_row // 2, width // 2, wd.shape[3]
    n_layers_b = wb.shape[0]
    n_group = n_dp * n_sp
    m_row = w_out * n_img
    my_pod, my_dp, my_sp = lax.axis_index("pod"), lax.axis_index("dp"), lax.axis_index("sp")
    me = my_dp * n_sp + my_sp
    is_top = my_sp == 0
    is_bottom = my_sp == n_sp - 1
    not_top = my_sp > 0
    not_bottom = my_sp < n_sp - 1
    upper = (my_pod, my_dp, lax.max(my_sp - 1, 0))
    lower = (my_pod, my_dp, lax.min(my_sp + 1, n_sp - 1))

    def peer(offset):
        flat = lax.rem(me + offset, n_group)
        return (my_pod, flat // n_sp, lax.rem(flat, n_sp))

    row_copies = [pltpu.make_async_copy(img.at[:, r], nat.at[r + 1], in_sem.at[r]) for r in range(n_row)]
    for c in row_copies:
        c.start()
    w_copies = []
    for p in range(3):
        for q in range(3):
            for half in range(2):
                k = q + half
                w_copies.append(pltpu.make_async_copy(
                    wa.at[p, q], wa_v.at[pl.ds(p * 4 * ch_a + k * ch_a, ch_a), pl.ds(half * ch_a, ch_a)],
                    w_sem.at[len(w_copies)]))
    for p in range(3):
        for q in range(3):
            off = p * 2 * ch_a + q * ch_a if q < 2 else 6 * ch_a + p * ch_a
            w_copies.append(pltpu.make_async_copy(wd.at[p, q], wd_v.at[pl.ds(off, ch_a)], w_sem.at[len(w_copies)]))
    w_copies.append(pltpu.make_async_copy(wb, wb_v, w_sem.at[len(w_copies)]))
    for c in w_copies:
        c.start()

    barrier = pltpu.get_barrier_semaphore()
    for i in range(1, n_group):
        pl.semaphore_signal(barrier, inc=1, device_id=peer(i), device_id_type=MESH)

    for p in range(3):
        wa_v[pl.ds(p * 4 * ch_a + 3 * ch_a, ch_a), 0:ch_a] = jnp.zeros((ch_a, ch_a), BF16)
        wa_v[pl.ds(p * 4 * ch_a, ch_a), ch_a:2 * ch_a] = jnp.zeros((ch_a, ch_a), BF16)
    n_rows_t = img_t.shape[0]
    img_t[:, 0, :, 0:ch_a] = jnp.zeros((n_rows_t, n_img, ch_a), BF16)
    img_t[:, w_out, :, ch_a:2 * ch_a] = jnp.zeros((n_rows_t, n_img, ch_a), BF16)
    act_a[:, w_out] = jnp.zeros((act_a.shape[0], n_img, 2 * ch_a), BF16)
    act_b[:, 0] = jnp.zeros((act_b.shape[0], n_img, ch_b), BF16)
    act_b[:, w_out + 1] = jnp.zeros((act_b.shape[0], n_img, ch_b), BF16)

    @pl.when(is_top)
    def _():
        nat[0] = jnp.zeros((n_img, width, ch_a), BF16)
        act_b[0] = jnp.zeros((w_out + 2, n_img, ch_b), BF16)

    @pl.when(is_bottom)
    def _():
        nat[n_row + 1] = jnp.zeros((n_img, width, ch_a), BF16)
        nat[n_row + 2] = jnp.zeros((n_img, width, ch_a), BF16)
        act_b[n_out_row + 1] = jnp.zeros((w_out + 2, n_img, ch_b), BF16)

    def image_halo(src_row, dst_row, dev, k):
        return pltpu.make_async_remote_copy(
            src_ref=img.at[:, src_row], dst_ref=nat.at[dst_row], send_sem=halo_in_send.at[k],
            recv_sem=halo_in_recv.at[k], device_id=dev, device_id_type=MESH)

    to_lower = image_halo(n_row - 1, 0, lower, 0)
    to_upper0 = image_halo(0, n_row + 1, upper, 1)
    cols_x = width * 4 // 7 // 16 * 16
    n_pair = cols_x // 2 - 1
    to_upper1 = pltpu.make_async_remote_copy(
        src_ref=img.at[:, 1, pl.ds(0, cols_x)], dst_ref=nat.at[n_row + 2, :, pl.ds(0, cols_x)], send_sem=halo_in_send.at[2],
        recv_sem=halo_in_recv.at[2], device_id=upper, device_id_type=MESH)
    far = pl.ds(n_pair * n_img, (w_out - n_pair) * n_img)
    to_upper_z = pltpu.make_async_remote_copy(
        src_ref=zbuf.at[0, far], dst_ref=zbuf.at[n_row, far], send_sem=halo_in_send.at[3],
        recv_sem=halo_in_recv.at[3], device_id=upper, device_id_type=MESH)

    def transpose_row(k, cols=width):
        pitch = stage.shape[0] // n_img

        for i in range(n_img):
            stage[pl.ds(i * pitch, cols), :] = nat[k, i, 0:cols].astype(F32)
        for x in range(cols):
            half = (x + 1) % 2
            img_t[k, (x + 1) // 2, :, half * ch_a:(half + 1) * ch_a] = (
                stage[pl.ds(x, n_img, stride=pitch), :].astype(BF16))

    def fold(total, z_val):
        z3 = z_val.reshape(z_val.shape[0] // 8, 8, ch_b)
        return total[0] + jnp.sum(z3, axis=0), total[1] + jnp.sum(z3 * z3, axis=0)

    def conv_a(r, rows=(0, 1, 2), pairs=w_out):
        parts = []
        for p in rows:
            for k in range(2):
                parts.append(img_t[r + p, pl.ds(k, pairs)].reshape(pairs * n_img, 2 * ch_a))
        w_val = wa_v[pl.ds(rows[0] * 4 * ch_a, len(rows) * 4 * ch_a)]
        return jnp.dot(jnp.concatenate(parts, axis=1), w_val, preferred_element_type=F32)

    def conv_down(r, first, count):
        m_val = count * n_img
        parts = [act_a[2 * r + p, pl.ds(first, count)].reshape(m_val, 2 * ch_a) for p in range(3)]
        parts += [act_a[2 * r + p, pl.ds(first + 1, count), :, 0:ch_a].reshape(m_val, ch_a) for p in range(3)]
        return jnp.dot(jnp.concatenate(parts, axis=1), wd_v[...], preferred_element_type=F32)

    def conv_b(r, layer, rows=(0, 1, 2), first=0, count=w_out):
        parts = []
        for p in rows:
            for q in range(3):
                parts.append(act_b[r + p, pl.ds(q + first, count)].reshape(count * n_img, ch_b))
        w_val = wb_v[layer, pl.ds(rows[0] * 3 * ch_b, len(rows) * 3 * ch_b)]
        return jnp.dot(jnp.concatenate(parts, axis=1), w_val, preferred_element_type=F32)

    def keep_z(r, z_val):
        zbuf[r] = z_val

    def keep_final(r, z_val, first=0):
        for x in range(z_val.shape[0] // n_img):
            for h in range(ch_b // 128):
                zfin[h, pl.ds((first + x) * n_img * n_out_row + r, n_img, stride=n_out_row), :] = (
                    z_val[x * n_img:(x + 1) * n_img, h * 128:(h + 1) * 128])

    def send_stats(layer, total):
        s1 = jnp.sum(total[0], axis=0, keepdims=True)
        s2 = jnp.sum(total[1], axis=0, keepdims=True)
        if layer == 0:
            s1 = s1[:, :ch_a] + s1[:, ch_a:]
            s2 = s2[:, :ch_a] + s2[:, ch_a:]
            s1 = jnp.concatenate([s1, s1], axis=1)
            s2 = jnp.concatenate([s2, s2], axis=1)
        both = jnp.concatenate([s1, s2], axis=0)
        stat_src[layer] = both
        last = layer == stat_src.shape[0] - 1
        slot = stat_out.at[me] if last else stat_dst.at[layer, me]
        if not last:
            stat_dst[layer, me] = both
        copies = []
        for i in range(1, n_group):
            copies.append(pltpu.make_async_remote_copy(
                src_ref=stat_src.at[layer], dst_ref=slot, send_sem=stat_send.at[layer, i],
                recv_sem=stat_recv.at[layer, i], device_id=peer(i), device_id_type=MESH))
        for c in copies:
            c.start()
        if last:
            copies.append(pltpu.make_async_copy(stat_src.at[layer], slot, own_sem))
            copies[-1].start()
        return copies

    def finish_stats(layer, copies, gamma, beta, count):
        with jax.named_scope("stats_wait"):
            for c in copies:
                c.wait()
        tot = jnp.sum(stat_dst[layer], axis=0)
        mean = tot[0:1] / count
        var = tot[1:2] / count - mean * mean
        scale = gamma * lax.rsqrt(var + EPS_VALUE)
        return scale, beta - mean * scale

    def normalize(z_val, coef):
        scale, shift = coef
        return jnp.maximum(z_val * scale + shift, 0.0).astype(BF16)

    def z_row(layer, r):
        return 2 * r + (layer + 1) % 2

    zeros = (jnp.zeros((8, ch_b), F32), jnp.zeros((8, ch_b), F32))

    def t_body(r, carry):
        pltpu.make_async_copy(img.at[:, r], nat.at[r + 1], in_sem.at[r]).wait()
        transpose_row(r + 1)
        return carry

    with jax.named_scope("transpose"):
        lax.fori_loop(0, n_row, t_body, 0)
    with jax.named_scope("barrier"):
        pl.semaphore_wait(barrier, n_group - 1)

    @pl.when(not_bottom)
    def _():
        to_lower.start()

    @pl.when(not_top)
    def _():
        to_upper0.start()
        to_upper1.start()

    for c in w_copies:
        c.wait()

    def a_body(i, total):
        r = 1 + 2 * i
        z_pair = [conv_a(r), conv_a(r + 1)]
        for j in range(2):
            keep_z(r + j, z_pair[j])
            total = fold(total, z_pair[j])
        return total

    with jax.named_scope("conv_a"):
        total = lax.fori_loop(0, (n_row - 4) // 2, a_body, zeros)
    with jax.named_scope("conv_a_part"):
        total = a_body((n_row - 4) // 2, total)
        keep_z(0, conv_a(0, (1, 2)))
        keep_z(n_row - 1, conv_a(n_row - 1, (0, 1)))
    with jax.named_scope("img_halo_wait"):
        @pl.when(not_top)
        def _():
            to_lower.wait_recv()

        @pl.when(not_bottom)
        def _():
            to_upper0.wait_recv()

    with jax.named_scope("transpose_halo"):
        transpose_row(0)
        transpose_row(n_row + 1)
    with jax.named_scope("conv_a_edge"):
        for r, p in ((0, 0), (n_row - 1, 2)):
            z_val = conv_a(r, (p,)) + zbuf[r]
            keep_z(r, z_val)
            total = fold(total, z_val)
    with jax.named_scope("send_stats"):
        copies = send_stats(0, total)

        @pl.when(not_top)
        def _():
            to_upper_z.start()

    with jax.named_scope("img_halo_wait2"):
        @pl.when(not_bottom)
        def _():
            to_upper1.wait_recv()

    with jax.named_scope("conv_a_extra"):
        transpose_row(n_row + 2, cols_x)
        zbuf[n_row, 0:n_pair * n_img] = conv_a(n_row, pairs=n_pair)
    n_a = float(n_group * n_img * n_row * width)
    wide = lambda v: jnp.concatenate([v, v], axis=1)
    coef_a = finish_stats(0, copies, wide(na[0, 0:1]), wide(na[0, 1:2]), n_a)

    n_piece = 3
    piece = w_out // n_piece

    def norm_a_cols(r, k):
        y_val = normalize(zbuf[r, k * piece * n_img:(k + 1) * piece * n_img], coef_a)
        if r == n_row:
            y_val = jnp.where(is_bottom, jnp.zeros_like(y_val), y_val)
        act_a[r, pl.ds(k * piece, piece)] = y_val.reshape(piece, n_img, 2 * ch_a)

    def norm_a_row(r):
        for k in range(n_piece):
            norm_a_cols(r, k)

    def down_cols(r, k, total):
        z_val = conv_down(r, k * piece, piece)
        zbuf[z_row(0, r), k * piece * n_img:(k + 1) * piece * n_img] = z_val
        return fold(total, z_val)

    with jax.named_scope("conv_down"):
        total = zeros
        for r in range(3):
            norm_a_row(r)
        for r in range(n_out_row - 1):
            for k in range(n_piece):
                norm_a_cols(2 * r + 3, k)
                if 2 * r + 4 < n_row:
                    norm_a_cols(2 * r + 4, k)
                total = down_cols(r, k, total)
    with jax.named_scope("down_halo_wait"):
        @pl.when(not_top)
        def _():
            to_upper_z.wait_send()

        @pl.when(not_bottom)
        def _():
            to_upper_z.wait_recv()

    with jax.named_scope("conv_down_last"):
        norm_a_row(n_row)
        for k in range(n_piece):
            total = down_cols(n_out_row - 1, k, total)

    late_cols = (n_early, (n_early + w_out) // 2, w_out)
    last_row = n_out_row - 1

    def early_copies(layer):
        slot = layer % 2
        up = pltpu.make_async_remote_copy(
            src_ref=zbuf.at[z_row(layer, 0), pl.ds(0, n_early * n_img)], dst_ref=zhalo.at[slot, 1], send_sem=early_send.at[layer, 1],
            recv_sem=early_recv.at[layer, 1], device_id=upper, device_id_type=MESH)
        down = pltpu.make_async_remote_copy(
            src_ref=zbuf.at[z_row(layer, last_row), pl.ds(0, n_early * n_img)], dst_ref=zhalo.at[slot, 0], send_sem=early_send.at[layer, 0],
            recv_sem=early_recv.at[layer, 0], device_id=lower, device_id_type=MESH)
        return up, down

    def late_copies(layer, k):
        cols = pl.ds(1 + late_cols[k], late_cols[k + 1] - late_cols[k])
        up = pltpu.make_async_remote_copy(
            src_ref=act_b.at[1, cols], dst_ref=act_b.at[n_out_row + 1, cols],
            send_sem=halo_send.at[layer, k, 1], recv_sem=halo_recv.at[layer, k, 1], device_id=upper, device_id_type=MESH)
        down = pltpu.make_async_remote_copy(
            src_ref=act_b.at[n_out_row, cols], dst_ref=act_b.at[0, cols],
            send_sem=halo_send.at[layer, k, 0], recv_sem=halo_recv.at[layer, k, 0], device_id=lower, device_id_type=MESH)
        return up, down

    def start_both(up, down):
        @pl.when(not_top)
        def _():
            up.start()

        @pl.when(not_bottom)
        def _():
            down.start()

    n_b = float(n_group * m_row * n_out_row)
    with jax.named_scope("send_stats"):
        copies = send_stats(1, total)
        up_early, down_early = early_copies(0)
        start_both(up_early, down_early)
    coef = finish_stats(1, copies, nd[0:1], nd[1:2], n_b)

    for layer in range(n_layers_b):
        def norm_b_cols(r, first, count):
            z_val = zbuf[z_row(layer, r), pl.ds(first * n_img, count * n_img)]
            act_b[r + 1, pl.ds(1 + first, count)] = normalize(z_val, coef).reshape(count, n_img, ch_b)

        late = [late_copies(layer, k) for k in range(2)]
        with jax.named_scope("norm_edge"):
            for k in range(2):
                norm_b_cols(0, late_cols[k], late_cols[k + 1] - late_cols[k])
                norm_b_cols(last_row, late_cols[k], late_cols[k + 1] - late_cols[k])
                start_both(*late[k])

        last = layer == n_layers_b - 1
        def keep(r, z_val):
            if last:
                keep_final(r, z_val)
            else:
                zbuf[z_row(layer + 1, r)] = z_val

        with jax.named_scope("conv_b_main"):
            norm_b_cols(0, 0, n_early)
            norm_b_cols(last_row, 0, n_early)
            for r in range(1, last_row):
                norm_b_cols(r, 0, w_out)
            total = zeros
            zbuf[z_row(layer + 1, 0)] = conv_b(0, layer, (1, 2))
            for r in range(1, last_row):
                z_val = conv_b(r, layer)
                keep(r, z_val)
                total = fold(total, z_val)
            zbuf[z_row(layer + 1, last_row)] = conv_b(last_row, layer, (0, 1))

        def keep_edge(r, z_val, first):
            if last:
                keep_final(r, z_val, first)
            else:
                zbuf[z_row(layer + 1, r), first * n_img:first * n_img + z_val.shape[0]] = z_val

        def edge_cols(first, count, total):
            rows = slice(first * n_img, (first + count) * n_img)
            for r, p in ((0, 0), (last_row, 2)):
                z_val = conv_b(r, layer, (p,), first, count) + zbuf[z_row(layer + 1, r), rows]
                keep_edge(r, z_val, first)
                total = fold(total, z_val)
            return total

        with jax.named_scope("halo_wait"):
            def norm_halo(side, row):
                y_val = normalize(zhalo[layer % 2, side], coef)
                act_b[row, pl.ds(1, n_early)] = y_val.reshape(n_early, n_img, ch_b)

            @pl.when(not_top)
            def _():
                up_early.wait_send()
                down_early.wait_recv()
                norm_halo(0, 0)
                late[0][0].wait_send()
                late[0][1].wait_recv()

            @pl.when(not_bottom)
            def _():
                down_early.wait_send()
                up_early.wait_recv()
                norm_halo(1, n_out_row + 1)
                late[0][1].wait_send()
                late[0][0].wait_recv()

        split = late_cols[1] - 1
        with jax.named_scope("conv_b_edge"):
            total = edge_cols(0, split, total)
        with jax.named_scope("halo_wait2"):
            @pl.when(not_top)
            def _():
                late[1][0].wait_send()
                late[1][1].wait_recv()

            @pl.when(not_bottom)
            def _():
                late[1][1].wait_send()
                late[1][0].wait_recv()

        with jax.named_scope("conv_b_edge2"):
            total = edge_cols(split, w_out - split, total)

        with jax.named_scope("send_stats"):
            copies = send_stats(2 + layer, total)
            if not last:
                up_early, down_early = early_copies(layer + 1)
                start_both(up_early, down_early)
        if not last:
            coef = finish_stats(2 + layer, copies, nb[layer, 0:1], nb[layer, 1:2], n_b)

    with jax.named_scope("z_out"):
        z_copy = pltpu.make_async_copy(zfin, z_out, out_sem)
        z_copy.start()
        z_copy.wait()
    with jax.named_scope("last_stats_wait"):
        for c in copies:
            c.wait()

    @pl.when(not_bottom)
    def _():
        to_lower.wait_send()

    @pl.when(not_top)
    def _():
        to_upper0.wait_send()
        to_upper1.wait_send()


def finish_kernel(count, z_hbm, stat_hbm, norm_hbm, out, z_v, stat, norms, out_v, z_sem, small_sem, out_sem):
    n_img, w_out, n_out_row, ch_b = out.shape
    n_chunk = z_sem.shape[0]
    chunk = w_out // n_chunk
    per_col = n_img * n_out_row

    def z_copy(k):
        rows = pl.ds(k * chunk * per_col, chunk * per_col)
        return pltpu.make_async_copy(z_hbm.at[:, rows], z_v.at[:, rows], z_sem.at[k])

    def out_copy(k):
        cols = pl.ds(k * chunk, chunk)
        return pltpu.make_async_copy(out_v.at[:, cols], out.at[:, cols], out_sem.at[k])

    small = [pltpu.make_async_copy(stat_hbm, stat, small_sem.at[0]), pltpu.make_async_copy(norm_hbm, norms, small_sem.at[1])]
    for c in small:
        c.start()
    for k in range(n_chunk):
        z_copy(k).start()
    for c in small:
        c.wait()
    norm = norms[norms.shape[0] - 1]
    tot = jnp.sum(stat[...], axis=0)
    mean = tot[0:1] / count
    var = tot[1:2] / count - mean * mean
    scale = norm[0:1] * lax.rsqrt(var + EPS_VALUE)
    shift = norm[1:2] - mean * scale
    for k in range(n_chunk):
        z_copy(k).wait()

        def out_body(x, carry):
            for h in range(ch_b // 128):
                lanes = slice(h * 128, (h + 1) * 128)
                z_val = z_v[h, pl.ds(x * per_col, per_col), :]
                y_val = jnp.maximum(z_val * scale[:, lanes] + shift[:, lanes], 0.0).astype(BF16)
                out_v[:, x, :, lanes] = y_val.reshape(n_img, n_out_row, 128)
            return carry

        lax.fori_loop(k * chunk, (k + 1) * chunk, out_body, 0, unroll=3)
        out_copy(k).start()
    for k in range(n_chunk):
        out_copy(k).wait()


def solution(mesh):
    n_sp, n_dp = mesh.shape['sp'], mesh.shape['dp']

    def local_stack(img, w_a, norm_a, w_down, norm_down, w_b, norm_b):
        n_img, n_row, width, ch_a = img.shape
        ch_b = w_down.shape[-1]
        n_out_row, w_out = n_row // 2, width // 2
        n_layers_b = w_b.shape[0]
        n_group = n_sp * n_dp
        any_spec = pl.BlockSpec(memory_space=pl.ANY)
        vmem_spec = pl.BlockSpec(memory_space=pltpu.VMEM)
        dma = pltpu.SemaphoreType.DMA
        n_stats = 2 + n_layers_b
        n_early = w_out // 3
        z_val, stats = pl.pallas_call(
            functools.partial(stack_kernel, n_dp, n_sp, n_early),
            out_shape=(
                jax.ShapeDtypeStruct((ch_b // 128, n_out_row * w_out * n_img, 128), F32),
                jax.ShapeDtypeStruct((n_group, 2, ch_b), F32),
            ),
            in_specs=[any_spec, any_spec, vmem_spec, any_spec, vmem_spec, any_spec, vmem_spec],
            out_specs=(any_spec, any_spec),
            scratch_shapes=[
                pltpu.VMEM((n_row + 3, n_img, width, ch_a), BF16),
                pltpu.VMEM((n_img * (width + 4), 128), F32),
                pltpu.VMEM((n_row + 3, w_out + 1, n_img, 2 * ch_a), BF16),
                pltpu.VMEM((n_row + 1, w_out + 1, n_img, 2 * ch_a), BF16),
                pltpu.VMEM((n_out_row + 2, w_out + 2, n_img, ch_b), BF16),
                pltpu.VMEM((n_row + 1, w_out * n_img, ch_b), F32),
                pltpu.VMEM((2, 2, n_early * n_img, ch_b), F32),
                pltpu.VMEM((ch_b // 128, n_out_row * w_out * n_img, 128), F32),
                pltpu.VMEM((12 * ch_a, ch_b), BF16),
                pltpu.VMEM((9 * ch_a, ch_b), BF16),
                pltpu.VMEM((n_layers_b, 9 * ch_b, ch_b), BF16),
                pltpu.VMEM((n_stats, 2, ch_b), F32),
                pltpu.VMEM((n_stats - 1, n_group, 2, ch_b), F32),
                dma((n_row,)), dma((28,)), dma((4,)), dma((4,)),
                dma((n_stats, n_group)), dma((n_stats, n_group)),
                dma((n_layers_b, 2, 2)), dma((n_layers_b, 2, 2)), dma((n_layers_b, 2)), dma((n_layers_b, 2)), dma, dma,
            ],
            compiler_params=pltpu.CompilerParams(
                collective_id=0, has_side_effects=True, vmem_limit_bytes=67043328),
        )(img, w_a[0], norm_a, w_down, norm_down, w_b.reshape(n_layers_b, 9 * ch_b, ch_b), norm_b)
        n_chunk = 4
        features = pl.pallas_call(
            functools.partial(finish_kernel, float(n_group * n_img * n_out_row * w_out)),
            out_shape=jax.ShapeDtypeStruct((n_img, w_out, n_out_row, ch_b), BF16),
            in_specs=[any_spec, any_spec, any_spec],
            out_specs=any_spec,
            scratch_shapes=[
                pltpu.VMEM(z_val.shape, F32),
                pltpu.VMEM(stats.shape, F32),
                pltpu.VMEM(norm_b.shape, F32),
                pltpu.VMEM((n_img, w_out, n_out_row, ch_b), BF16),
                dma((n_chunk,)), dma((2,)), dma((n_chunk,)),
            ],
            compiler_params=pltpu.CompilerParams(vmem_limit_bytes=67043328),
        )(z_val, stats, norm_b)
        return features.transpose(0, 2, 1, 3)

    act_spec = P(('pod', 'dp'), 'sp', None, None)
    return jax.shard_map(local_stack, mesh=mesh, in_specs=(act_spec, P(), P(), P(), P(), P(), P()), out_specs=act_spec, check_vma=False)
```

```python
import functools

import jax
import jax.numpy as jnp
from jax import lax
from jax.experimental import pallas as pl
from jax.experimental.pallas import tpu as pltpu
from jax.sharding import PartitionSpec as P

EPS_VALUE = 1e-5
MESH = pl.DeviceIdType.MESH
BF16 = jnp.bfloat16
F32 = jnp.float32


def stack_kernel(n_dp, n_sp, n_early, img, wa, na, wd, nd, wb, nb, z_out, stat_out,
                 nat, stage, img_t, act_a, act_b, zbuf, zhalo, zfin,
                 wa_v, wd_v, wb_v, stat_src, stat_dst,
                 in_sem, w_sem, halo_in_send, halo_in_recv, stat_send, stat_recv,
                 halo_send, halo_recv, early_send, early_recv, out_sem, own_sem):
    n_img, n_row, width, ch_a = img.shape
    n_out_row, w_out, ch_b = n_row // 2, width // 2, wd.shape[3]
    n_layers_b = wb.shape[0]
    n_group = n_dp * n_sp
    m_row = w_out * n_img
    my_pod, my_dp, my_sp = lax.axis_index("pod"), lax.axis_index("dp"), lax.axis_index("sp")
    me = my_dp * n_sp + my_sp
    is_top = my_sp == 0
    is_bottom = my_sp == n_sp - 1
    not_top = my_sp > 0
    not_bottom = my_sp < n_sp - 1
    upper = (my_pod, my_dp, lax.max(my_sp - 1, 0))
    lower = (my_pod, my_dp, lax.min(my_sp + 1, n_sp - 1))

    def peer(offset):
        flat = lax.rem(me + offset, n_group)
        return (my_pod, flat // n_sp, lax.rem(flat, n_sp))

    barrier = pltpu.get_barrier_semaphore()
    for i in range(1, n_group):
        pl.semaphore_signal(barrier, inc=1, device_id=peer(i), device_id_type=MESH)

    row_copies = [pltpu.make_async_copy(img.at[:, r], nat.at[r + 1], in_sem.at[r]) for r in range(n_row)]
    for c in row_copies:
        c.start()
    w_copies = []
    for p in range(3):
        for q in range(3):
            for half in range(2):
                k = q + half
                w_copies.append(pltpu.make_async_copy(
                    wa.at[p, q], wa_v.at[pl.ds(p * 4 * ch_a + k * ch_a, ch_a), pl.ds(half * ch_a, ch_a)],
                    w_sem.at[len(w_copies)]))
    for p in range(3):
        for q in range(3):
            off = p * 2 * ch_a + q * ch_a if q < 2 else 6 * ch_a + p * ch_a
            w_copies.append(pltpu.make_async_copy(wd.at[p, q], wd_v.at[pl.ds(off, ch_a)], w_sem.at[len(w_copies)]))
    w_copies.append(pltpu.make_async_copy(wb, wb_v, w_sem.at[len(w_copies)]))
    for c in w_copies:
        c.start()

    for p in range(3):
        wa_v[pl.ds(p * 4 * ch_a + 3 * ch_a, ch_a), 0:ch_a] = jnp.zeros((ch_a, ch_a), BF16)
        wa_v[pl.ds(p * 4 * ch_a, ch_a), ch_a:2 * ch_a] = jnp.zeros((ch_a, ch_a), BF16)
    n_rows_t = img_t.shape[0]
    img_t[:, 0, :, 0:ch_a] = jnp.zeros((n_rows_t, n_img, ch_a), BF16)
    img_t[:, w_out, :, ch_a:2 * ch_a] = jnp.zeros((n_rows_t, n_img, ch_a), BF16)
    act_a[:, w_out] = jnp.zeros((act_a.shape[0], n_img, 2 * ch_a), BF16)
    act_b[:, 0] = jnp.zeros((act_b.shape[0], n_img, ch_b), BF16)
    act_b[:, w_out + 1] = jnp.zeros((act_b.shape[0], n_img, ch_b), BF16)

    @pl.when(is_top)
    def _():
        nat[0] = jnp.zeros((n_img, width, ch_a), BF16)
        act_b[0] = jnp.zeros((w_out + 2, n_img, ch_b), BF16)

    @pl.when(is_bottom)
    def _():
        nat[n_row + 1] = jnp.zeros((n_img, width, ch_a), BF16)
        nat[n_row + 2] = jnp.zeros((n_img, width, ch_a), BF16)
        act_b[n_out_row + 1] = jnp.zeros((w_out + 2, n_img, ch_b), BF16)
        act_a[n_row] = jnp.zeros((w_out + 1, n_img, 2 * ch_a), BF16)

    x_split = width * 4 // 7 // 16 * 16
    cols_x = width * 10 // 21 // 16 * 16
    n_pair = cols_x // 2 - 1
    n_far = n_pair + w_out * 22 // 84

    def remote(src, dst, k, dev):
        return pltpu.make_async_remote_copy(
            src_ref=src, dst_ref=dst, send_sem=halo_in_send.at[k], recv_sem=halo_in_recv.at[k],
            device_id=dev, device_id_type=MESH)

    def image_halo(src_row, dst_row, dev, k, first, count):
        cols = pl.ds(first, count)
        return remote(nat.at[src_row + 1, :, cols], nat.at[dst_row, :, cols], k, dev)

    x_parts = ((0, x_split), (x_split, width - x_split))
    to_lower = [image_halo(n_row - 1, 0, lower, k, *x_parts[k]) for k in range(2)]
    to_upper = [image_halo(0, n_row + 1, upper, 2 + k, *x_parts[k]) for k in range(2)]
    to_upper.append(image_halo(1, n_row + 2, upper, 4, 0, cols_x))
    mid = pl.ds(n_pair * n_img, (n_far - n_pair) * n_img)
    to_upper_z = remote(zbuf.at[0, mid], zbuf.at[n_row, mid], 5, upper)
    far = pl.ds(n_far, w_out - n_far)
    to_upper_y = remote(act_a.at[0, far], act_a.at[n_row, far], 6, upper)

    def transpose_row(k, first=0, cols=width):
        pitch = stage.shape[0] // n_img

        for i in range(n_img):
            stage[pl.ds(i * pitch + first, cols), :] = nat[k, i, first:first + cols].astype(F32)
        for x in range(first, first + cols):
            half = (x + 1) % 2
            img_t[k, (x + 1) // 2, :, half * ch_a:(half + 1) * ch_a] = (
                stage[pl.ds(x, n_img, stride=pitch), :].astype(BF16))

    def fold(total, z_val):
        z3 = z_val.reshape(z_val.shape[0] // 8, 8, ch_b)
        return total[0] + jnp.sum(z3, axis=0), total[1] + jnp.sum(z3 * z3, axis=0)

    def conv_a(r, rows=(0, 1, 2), first=0, pairs=w_out):
        parts = []
        for p in rows:
            for k in range(2):
                parts.append(img_t[r + p, pl.ds(k + first, pairs)].reshape(pairs * n_img, 2 * ch_a))
        w_val = wa_v[pl.ds(rows[0] * 4 * ch_a, len(rows) * 4 * ch_a)]
        return jnp.dot(jnp.concatenate(parts, axis=1), w_val, preferred_element_type=F32)

    def conv_down(r, first, count):
        m_val = count * n_img
        parts = [act_a[2 * r + p, pl.ds(first, count)].reshape(m_val, 2 * ch_a) for p in range(3)]
        parts += [act_a[2 * r + p, pl.ds(first + 1, count), :, 0:ch_a].reshape(m_val, ch_a) for p in range(3)]
        return jnp.dot(jnp.concatenate(parts, axis=1), wd_v[...], preferred_element_type=F32)

    def conv_b(r, layer, rows=(0, 1, 2), first=0, count=w_out):
        parts = []
        for p in rows:
            for q in range(3):
                parts.append(act_b[r + p, pl.ds(q + first, count)].reshape(count * n_img, ch_b))
        w_val = wb_v[layer, pl.ds(rows[0] * 3 * ch_b, len(rows) * 3 * ch_b)]
        return jnp.dot(jnp.concatenate(parts, axis=1), w_val, preferred_element_type=F32)

    def keep_z(r, z_val):
        zbuf[r] = z_val

    def keep_final(r, z_val, first=0):
        for x in range(z_val.shape[0] // n_img):
            for h in range(ch_b // 128):
                zfin[h, pl.ds((first + x) * n_img * n_out_row + r, n_img, stride=n_out_row), :] = (
                    z_val[x * n_img:(x + 1) * n_img, h * 128:(h + 1) * 128])

    def send_stats(layer, total):
        s1 = jnp.sum(total[0], axis=0, keepdims=True)
        s2 = jnp.sum(total[1], axis=0, keepdims=True)
        if layer == 0:
            s1 = s1[:, :ch_a] + s1[:, ch_a:]
            s2 = s2[:, :ch_a] + s2[:, ch_a:]
            s1 = jnp.concatenate([s1, s1], axis=1)
            s2 = jnp.concatenate([s2, s2], axis=1)
        both = jnp.concatenate([s1, s2], axis=0)
        stat_src[layer] = both
        last = layer == stat_src.shape[0] - 1
        slot = stat_out.at[me] if last else stat_dst.at[layer, me]
        if not last:
            stat_dst[layer, me] = both
        copies = []
        for i in range(1, n_group):
            copies.append(pltpu.make_async_remote_copy(
                src_ref=stat_src.at[layer], dst_ref=slot, send_sem=stat_send.at[layer, i],
                recv_sem=stat_recv.at[layer, i], device_id=peer(i), device_id_type=MESH))
        for c in copies:
            c.start()
        if last:
            copies.append(pltpu.make_async_copy(stat_src.at[layer], slot, own_sem))
            copies[-1].start()
        return copies

    def finish_stats(layer, copies, gamma, beta, count):
        with jax.named_scope("stats_wait"):
            for c in copies:
                c.wait()
        tot = jnp.sum(stat_dst[layer], axis=0)
        mean = tot[0:1] / count
        var = tot[1:2] / count - mean * mean
        scale = gamma * lax.rsqrt(var + EPS_VALUE)
        return scale, beta - mean * scale

    def normalize(z_val, coef):
        scale, shift = coef
        return jnp.maximum(z_val * scale + shift, 0.0).astype(BF16)

    def z_row(layer, r):
        return 2 * r + (layer + 1) % 2

    zeros = (jnp.zeros((8, ch_b), F32), jnp.zeros((8, ch_b), F32))

    def t_body(r, carry):
        pltpu.make_async_copy(img.at[:, r], nat.at[r + 1], in_sem.at[r]).wait()
        transpose_row(r + 1)
        return carry

    with jax.named_scope("transpose"):
        lax.fori_loop(0, n_row, t_body, 0)
    for c in w_copies[:18]:
        c.wait()

    def a_rows(first, count, total):
        z_rows = [conv_a(first + j) for j in range(count)]
        for j in range(count):
            keep_z(first + j, z_rows[j])
            total = fold(total, z_rows[j])
        return total

    with jax.named_scope("barrier"):
        pl.semaphore_wait(barrier, n_group - 1)

    @pl.when(not_bottom)
    def _():
        for c in to_lower:
            c.start()

    @pl.when(not_top)
    def _():
        for c in to_upper:
            c.start()

    with jax.named_scope("conv_a_first"):
        total = a_rows(1, 1, zeros)
    with jax.named_scope("conv_a"):
        total = lax.fori_loop(0, (n_row - 4) // 2, lambda i, t: a_rows(2 + 2 * i, 2, t), total)
    with jax.named_scope("conv_a_part"):
        total = a_rows(n_row - 2, 1, total)
        keep_z(0, conv_a(0, (1, 2)))
        keep_z(n_row - 1, conv_a(n_row - 1, (0, 1)))

    pair_parts = ((0, (x_split - 1) // 2), ((x_split - 1) // 2, w_out - (x_split - 1) // 2))
    for k in range(2):
        with jax.named_scope("img_halo_wait"):
            @pl.when(not_top)
            def _():
                to_lower[k].wait_recv()

            @pl.when(not_bottom)
            def _():
                to_upper[k].wait_recv()

        with jax.named_scope("transpose_halo"):
            transpose_row(0, *x_parts[k])
            transpose_row(n_row + 1, *x_parts[k])
        with jax.named_scope("conv_a_edge"):
            first, count = pair_parts[k]
            rows = slice(first * n_img, (first + count) * n_img)
            for r, p in ((0, 0), (n_row - 1, 2)):
                z_val = conv_a(r, (p,), first, count) + zbuf[r, rows]
                zbuf[r, rows] = z_val
                total = fold(total, z_val)
    with jax.named_scope("send_stats"):
        copies = send_stats(0, total)

        @pl.when(not_top)
        def _():
            to_upper_z.start()

    for c in w_copies[18:]:
        c.wait()
    with jax.named_scope("img_halo_wait2"):
        @pl.when(not_bottom)
        def _():
            to_upper[2].wait_recv()

    with jax.named_scope("conv_a_extra"):
        transpose_row(n_row + 2, 0, cols_x)
        zbuf[n_row, 0:n_pair * n_img] = conv_a(n_row, pairs=n_pair)
    n_a = float(n_group * n_img * n_row * width)
    wide = lambda v: jnp.concatenate([v, v], axis=1)
    coef_a = finish_stats(0, copies, wide(na[0, 0:1]), wide(na[0, 1:2]), n_a)

    n_piece = 3
    piece = w_out // n_piece

    def norm_a_cols(r, k):
        y_val = normalize(zbuf[r, k * piece * n_img:(k + 1) * piece * n_img], coef_a)
        act_a[r, pl.ds(k * piece, piece)] = y_val.reshape(piece, n_img, 2 * ch_a)

    def norm_a_row(r):
        for k in range(n_piece):
            norm_a_cols(r, k)

    def down_cols(r, k, total):
        z_val = conv_down(r, k * piece, piece)
        zbuf[z_row(0, r), k * piece * n_img:(k + 1) * piece * n_img] = z_val
        return fold(total, z_val)

    with jax.named_scope("conv_down"):
        total = zeros
        norm_a_row(0)

        @pl.when(not_top)
        def _():
            to_upper_y.start()

        for r in range(1, 3):
            norm_a_row(r)
        for r in range(n_out_row - 1):
            for k in range(n_piece):
                norm_a_cols(2 * r + 3, k)
                if 2 * r + 4 < n_row:
                    norm_a_cols(2 * r + 4, k)
                total = down_cols(r, k, total)
    with jax.named_scope("down_halo_wait"):
        @pl.when(not_top)
        def _():
            to_upper_z.wait_send()
            to_upper_y.wait_send()

        @pl.when(not_bottom)
        def _():
            to_upper_z.wait_recv()
            to_upper_y.wait_recv()

    with jax.named_scope("conv_down_last"):
        y_val = normalize(zbuf[n_row, 0:n_far * n_img], coef_a)
        y_val = jnp.where(is_bottom, jnp.zeros_like(y_val), y_val)
        act_a[n_row, pl.ds(0, n_far)] = y_val.reshape(n_far, n_img, 2 * ch_a)
        for k in range(n_piece):
            total = down_cols(n_out_row - 1, k, total)

    late_cols = (n_early, (n_early + 2 * w_out) // 3, w_out)
    last_row = n_out_row - 1

    def early_copies(layer):
        slot = layer % 2
        up = pltpu.make_async_remote_copy(
            src_ref=zbuf.at[z_row(layer, 0), pl.ds(0, n_early * n_img)], dst_ref=zhalo.at[slot, 1], send_sem=early_send.at[layer, 1],
            recv_sem=early_recv.at[layer, 1], device_id=upper, device_id_type=MESH)
        down = pltpu.make_async_remote_copy(
            src_ref=zbuf.at[z_row(layer, last_row), pl.ds(0, n_early * n_img)], dst_ref=zhalo.at[slot, 0], send_sem=early_send.at[layer, 0],
            recv_sem=early_recv.at[layer, 0], device_id=lower, device_id_type=MESH)
        return up, down

    def late_copies(layer, k):
        cols = pl.ds(1 + late_cols[k], late_cols[k + 1] - late_cols[k])
        up = pltpu.make_async_remote_copy(
            src_ref=act_b.at[1, cols], dst_ref=act_b.at[n_out_row + 1, cols],
            send_sem=halo_send.at[layer, k, 1], recv_sem=halo_recv.at[layer, k, 1], device_id=upper, device_id_type=MESH)
        down = pltpu.make_async_remote_copy(
            src_ref=act_b.at[n_out_row, cols], dst_ref=act_b.at[0, cols],
            send_sem=halo_send.at[layer, k, 0], recv_sem=halo_recv.at[layer, k, 0], device_id=lower, device_id_type=MESH)
        return up, down

    def start_both(up, down):
        @pl.when(not_top)
        def _():
            up.start()

        @pl.when(not_bottom)
        def _():
            down.start()

    n_b = float(n_group * m_row * n_out_row)
    with jax.named_scope("send_stats"):
        copies = send_stats(1, total)
        up_early, down_early = early_copies(0)
        start_both(up_early, down_early)
    coef = finish_stats(1, copies, nd[0:1], nd[1:2], n_b)

    for layer in range(n_layers_b):
        def norm_b_cols(r, first, count):
            z_val = zbuf[z_row(layer, r), pl.ds(first * n_img, count * n_img)]
            act_b[r + 1, pl.ds(1 + first, count)] = normalize(z_val, coef).reshape(count, n_img, ch_b)

        late = [late_copies(layer, k) for k in range(2)]
        with jax.named_scope("norm_edge"):
            for k in range(2):
                norm_b_cols(0, late_cols[k], late_cols[k + 1] - late_cols[k])
                norm_b_cols(last_row, late_cols[k], late_cols[k + 1] - late_cols[k])
                start_both(*late[k])

        last = layer == n_layers_b - 1
        def keep(r, z_val):
            if last:
                keep_final(r, z_val)
            else:
                zbuf[z_row(layer + 1, r)] = z_val

        with jax.named_scope("conv_b_main"):
            norm_b_cols(0, 0, n_early)
            norm_b_cols(last_row, 0, n_early)
            for r in range(1, last_row):
                norm_b_cols(r, 0, w_out)
            total = zeros
            zbuf[z_row(layer + 1, 0)] = conv_b(0, layer, (1, 2))
            for r in range(1, last_row):
                z_val = conv_b(r, layer)
                keep(r, z_val)
                total = fold(total, z_val)
            zbuf[z_row(layer + 1, last_row)] = conv_b(last_row, layer, (0, 1))

        def keep_edge(r, z_val, first):
            if last:
                keep_final(r, z_val, first)
            else:
                zbuf[z_row(layer + 1, r), first * n_img:first * n_img + z_val.shape[0]] = z_val

        def edge_cols(first, count, total):
            rows = slice(first * n_img, (first + count) * n_img)
            for r, p in ((0, 0), (last_row, 2)):
                z_val = conv_b(r, layer, (p,), first, count) + zbuf[z_row(layer + 1, r), rows]
                keep_edge(r, z_val, first)
                total = fold(total, z_val)
            return total

        with jax.named_scope("halo_wait"):
            def norm_halo(side, row):
                y_val = normalize(zhalo[layer % 2, side], coef)
                act_b[row, pl.ds(1, n_early)] = y_val.reshape(n_early, n_img, ch_b)

            @pl.when(not_top)
            def _():
                up_early.wait_send()
                down_early.wait_recv()
                norm_halo(0, 0)
                late[0][0].wait_send()
                late[0][1].wait_recv()

            @pl.when(not_bottom)
            def _():
                down_early.wait_send()
                up_early.wait_recv()
                norm_halo(1, n_out_row + 1)
                late[0][1].wait_send()
                late[0][0].wait_recv()

        split = late_cols[1] - 1
        with jax.named_scope("conv_b_edge"):
            total = edge_cols(0, split, total)
        with jax.named_scope("halo_wait2"):
            @pl.when(not_top)
            def _():
                late[1][0].wait_send()
                late[1][1].wait_recv()

            @pl.when(not_bottom)
            def _():
                late[1][1].wait_send()
                late[1][0].wait_recv()

        with jax.named_scope("conv_b_edge2"):
            total = edge_cols(split, w_out - split, total)

        with jax.named_scope("send_stats"):
            copies = send_stats(2 + layer, total)
            if not last:
                up_early, down_early = early_copies(layer + 1)
                start_both(up_early, down_early)
        if not last:
            coef = finish_stats(2 + layer, copies, nb[layer, 0:1], nb[layer, 1:2], n_b)

    with jax.named_scope("z_out"):
        z_copy = pltpu.make_async_copy(zfin, z_out, out_sem)
        z_copy.start()
        z_copy.wait()
    with jax.named_scope("last_stats_wait"):
        for c in copies:
            c.wait()

    @pl.when(not_bottom)
    def _():
        for c in to_lower:
            c.wait_send()

    @pl.when(not_top)
    def _():
        for c in to_upper:
            c.wait_send()


def finish_kernel(count, z_hbm, stat_hbm, norm_hbm, out, z_v, stat, norms, out_v, z_sem, small_sem, out_sem):
    n_img, w_out, n_out_row, ch_b = out.shape
    n_chunk = z_sem.shape[0]
    chunk = w_out // n_chunk
    per_col = n_img * n_out_row

    def z_copy(k):
        rows = pl.ds(k * chunk * per_col, chunk * per_col)
        return pltpu.make_async_copy(z_hbm.at[:, rows], z_v.at[:, rows], z_sem.at[k])

    def out_copy(k):
        cols = pl.ds(k * chunk, chunk)
        return pltpu.make_async_copy(out_v.at[:, cols], out.at[:, cols], out_sem.at[k])

    small = [pltpu.make_async_copy(stat_hbm, stat, small_sem.at[0]), pltpu.make_async_copy(norm_hbm, norms, small_sem.at[1])]
    for c in small:
        c.start()
    for k in range(n_chunk):
        z_copy(k).start()
    for c in small:
        c.wait()
    norm = norms[norms.shape[0] - 1]
    tot = jnp.sum(stat[...], axis=0)
    mean = tot[0:1] / count
    var = tot[1:2] / count - mean * mean
    scale = norm[0:1] * lax.rsqrt(var + EPS_VALUE)
    shift = norm[1:2] - mean * scale
    for k in range(n_chunk):
        z_copy(k).wait()

        def out_body(x, carry):
            for h in range(ch_b // 128):
                lanes = slice(h * 128, (h + 1) * 128)
                z_val = z_v[h, pl.ds(x * per_col, per_col), :]
                y_val = jnp.maximum(z_val * scale[:, lanes] + shift[:, lanes], 0.0).astype(BF16)
                out_v[:, x, :, lanes] = y_val.reshape(n_img, n_out_row, 128)
            return carry

        lax.fori_loop(k * chunk, (k + 1) * chunk, out_body, 0, unroll=3)
        out_copy(k).start()
    for k in range(n_chunk):
        out_copy(k).wait()


def solution(mesh):
    n_sp, n_dp = mesh.shape['sp'], mesh.shape['dp']

    def local_stack(img, w_a, norm_a, w_down, norm_down, w_b, norm_b):
        n_img, n_row, width, ch_a = img.shape
        ch_b = w_down.shape[-1]
        n_out_row, w_out = n_row // 2, width // 2
        n_layers_b = w_b.shape[0]
        n_group = n_sp * n_dp
        any_spec = pl.BlockSpec(memory_space=pl.ANY)
        vmem_spec = pl.BlockSpec(memory_space=pltpu.VMEM)
        dma = pltpu.SemaphoreType.DMA
        n_stats = 2 + n_layers_b
        n_early = w_out // 4
        z_val, stats = pl.pallas_call(
            functools.partial(stack_kernel, n_dp, n_sp, n_early),
            out_shape=(
                jax.ShapeDtypeStruct((ch_b // 128, n_out_row * w_out * n_img, 128), F32),
                jax.ShapeDtypeStruct((n_group, 2, ch_b), F32),
            ),
            in_specs=[any_spec, any_spec, vmem_spec, any_spec, vmem_spec, any_spec, vmem_spec],
            out_specs=(any_spec, any_spec),
            scratch_shapes=[
                pltpu.VMEM((n_row + 3, n_img, width, ch_a), BF16),
                pltpu.VMEM((n_img * (width + 4), 128), F32),
                pltpu.VMEM((n_row + 3, w_out + 1, n_img, 2 * ch_a), BF16),
                pltpu.VMEM((n_row + 1, w_out + 1, n_img, 2 * ch_a), BF16),
                pltpu.VMEM((n_out_row + 2, w_out + 2, n_img, ch_b), BF16),
                pltpu.VMEM((n_row + 1, w_out * n_img, ch_b), F32),
                pltpu.VMEM((2, 2, n_early * n_img, ch_b), F32),
                pltpu.VMEM((ch_b // 128, n_out_row * w_out * n_img, 128), F32),
                pltpu.VMEM((12 * ch_a, ch_b), BF16),
                pltpu.VMEM((9 * ch_a, ch_b), BF16),
                pltpu.VMEM((n_layers_b, 9 * ch_b, ch_b), BF16),
                pltpu.VMEM((n_stats, 2, ch_b), F32),
                pltpu.VMEM((n_stats - 1, n_group, 2, ch_b), F32),
                dma((n_row,)), dma((28,)), dma((7,)), dma((7,)),
                dma((n_stats, n_group)), dma((n_stats, n_group)),
                dma((n_layers_b, 2, 2)), dma((n_layers_b, 2, 2)), dma((n_layers_b, 2)), dma((n_layers_b, 2)), dma, dma,
            ],
            compiler_params=pltpu.CompilerParams(
                collective_id=0, has_side_effects=True, vmem_limit_bytes=67043328),
        )(img, w_a[0], norm_a, w_down, norm_down, w_b.reshape(n_layers_b, 9 * ch_b, ch_b), norm_b)
        n_chunk = 4
        features = pl.pallas_call(
            functools.partial(finish_kernel, float(n_group * n_img * n_out_row * w_out)),
            out_shape=jax.ShapeDtypeStruct((n_img, w_out, n_out_row, ch_b), BF16),
            in_specs=[any_spec, any_spec, any_spec],
            out_specs=any_spec,
            scratch_shapes=[
                pltpu.VMEM(z_val.shape, F32),
                pltpu.VMEM(stats.shape, F32),
                pltpu.VMEM(norm_b.shape, F32),
                pltpu.VMEM((n_img, w_out, n_out_row, ch_b), BF16),
                dma((n_chunk,)), dma((2,)), dma((n_chunk,)),
            ],
            compiler_params=pltpu.CompilerParams(vmem_limit_bytes=67043328),
        )(z_val, stats, norm_b)
        return features.transpose(0, 2, 1, 3)

    act_spec = P(('pod', 'dp'), 'sp', None, None)
    return jax.shard_map(local_stack, mesh=mesh, in_specs=(act_spec, P(), P(), P(), P(), P(), P()), out_specs=act_spec, check_vma=False)
```

```python
import functools

import jax
import jax.numpy as jnp
from jax import lax
from jax.experimental import pallas as pl
from jax.experimental.pallas import tpu as pltpu
from jax.sharding import PartitionSpec as P

EPS_VALUE = 1e-5
MESH = pl.DeviceIdType.MESH
BF16 = jnp.bfloat16
F32 = jnp.float32


def stack_kernel(n_dp, n_sp, n_early, img, wa, na, wd, nd, wb, nb, z_out, stat_out,
                 nat, stage, img_t, act_a, act_b, zbuf, zhalo, zfin,
                 wa_v, wd_v, wb_v, stat_src, stat_dst,
                 in_sem, w_sem, halo_in_send, halo_in_recv, stat_send, stat_recv,
                 halo_send, halo_recv, early_send, early_recv, out_sem, own_sem):
    n_img, n_row, width, ch_a = img.shape
    n_out_row, w_out, ch_b = n_row // 2, width // 2, wd.shape[3]
    n_layers_b = wb.shape[0]
    n_group = n_dp * n_sp
    m_row = w_out * n_img
    my_pod, my_dp, my_sp = lax.axis_index("pod"), lax.axis_index("dp"), lax.axis_index("sp")
    me = my_dp * n_sp + my_sp
    is_top = my_sp == 0
    is_bottom = my_sp == n_sp - 1
    not_top = my_sp > 0
    not_bottom = my_sp < n_sp - 1
    upper = (my_pod, my_dp, lax.max(my_sp - 1, 0))
    lower = (my_pod, my_dp, lax.min(my_sp + 1, n_sp - 1))

    def peer(offset):
        flat = lax.rem(me + offset, n_group)
        return (my_pod, flat // n_sp, lax.rem(flat, n_sp))

    barrier = pltpu.get_barrier_semaphore()
    for i in range(1, n_group):
        pl.semaphore_signal(barrier, inc=1, device_id=peer(i), device_id_type=MESH)

    row_copies = [pltpu.make_async_copy(img.at[:, r], nat.at[r + 1], in_sem.at[r]) for r in range(n_row)]
    for c in row_copies:
        c.start()
    w_copies = []
    for p in range(3):
        for q in range(3):
            for half in range(2):
                k = q + half
                w_copies.append(pltpu.make_async_copy(
                    wa.at[p, q], wa_v.at[pl.ds(p * 4 * ch_a + k * ch_a, ch_a), pl.ds(half * ch_a, ch_a)],
                    w_sem.at[0]))
    for p in range(3):
        for q in range(3):
            off = p * 2 * ch_a + q * ch_a if q < 2 else 6 * ch_a + p * ch_a
            w_copies.append(pltpu.make_async_copy(wd.at[p, q], wd_v.at[pl.ds(off, ch_a)], w_sem.at[1]))
    w_copies.append(pltpu.make_async_copy(wb, wb_v, w_sem.at[2]))
    for c in w_copies:
        c.start()

    for p in range(3):
        wa_v[pl.ds(p * 4 * ch_a + 3 * ch_a, ch_a), 0:ch_a] = jnp.zeros((ch_a, ch_a), BF16)
        wa_v[pl.ds(p * 4 * ch_a, ch_a), ch_a:2 * ch_a] = jnp.zeros((ch_a, ch_a), BF16)
    n_rows_t = img_t.shape[0]
    img_t[:, 0, :, 0:ch_a] = jnp.zeros((n_rows_t, n_img, ch_a), BF16)
    img_t[:, w_out, :, ch_a:2 * ch_a] = jnp.zeros((n_rows_t, n_img, ch_a), BF16)
    act_a[:, w_out] = jnp.zeros((act_a.shape[0], n_img, 2 * ch_a), BF16)
    act_b[:, 0] = jnp.zeros((act_b.shape[0], n_img, ch_b), BF16)
    act_b[:, w_out + 1] = jnp.zeros((act_b.shape[0], n_img, ch_b), BF16)

    @pl.when(is_top)
    def _():
        nat[0] = jnp.zeros((n_img, width, ch_a), BF16)
        act_b[0] = jnp.zeros((w_out + 2, n_img, ch_b), BF16)

    @pl.when(is_bottom)
    def _():
        nat[n_row + 1] = jnp.zeros((n_img, width, ch_a), BF16)
        nat[n_row + 2] = jnp.zeros((n_img, width, ch_a), BF16)
        act_b[n_out_row + 1] = jnp.zeros((w_out + 2, n_img, ch_b), BF16)
        act_a[n_row] = jnp.zeros((w_out + 1, n_img, 2 * ch_a), BF16)

    x_split = width * 4 // 7 // 16 * 16
    cols_x = width * 10 // 21 // 16 * 16
    n_pair = cols_x // 2 - 1
    n_far = n_pair + w_out * 22 // 84

    def remote(src, dst, k, dev):
        return pltpu.make_async_remote_copy(
            src_ref=src, dst_ref=dst, send_sem=halo_in_send.at[k], recv_sem=halo_in_recv.at[k],
            device_id=dev, device_id_type=MESH)

    def image_halo(src_row, dst_row, dev, k, first, count):
        cols = pl.ds(first, count)
        return remote(nat.at[src_row + 1, :, cols], nat.at[dst_row, :, cols], k, dev)

    x_parts = ((0, x_split), (x_split, width - x_split))
    to_lower = [image_halo(n_row - 1, 0, lower, k, *x_parts[k]) for k in range(2)]
    to_upper = [image_halo(0, n_row + 1, upper, 2 + k, *x_parts[k]) for k in range(2)]
    to_upper.append(image_halo(1, n_row + 2, upper, 4, 0, cols_x))
    mid = pl.ds(n_pair * n_img, (n_far - n_pair) * n_img)
    to_upper_z = remote(zbuf.at[0, mid], zbuf.at[n_row, mid], 5, upper)
    far = pl.ds(n_far, w_out - n_far)
    to_upper_y = remote(act_a.at[0, far], act_a.at[n_row, far], 6, upper)

    def transpose_row(k, first=0, cols=width):
        pitch = stage.shape[0] // n_img

        for i in range(n_img):
            stage[pl.ds(i * pitch + first, cols), :] = nat[k, i, first:first + cols].astype(F32)
        for x in range(first, first + cols):
            half = (x + 1) % 2
            img_t[k, (x + 1) // 2, :, half * ch_a:(half + 1) * ch_a] = (
                stage[pl.ds(x, n_img, stride=pitch), :].astype(BF16))

    def fold(total, z_val):
        z3 = z_val.reshape(z_val.shape[0] // 8, 8, ch_b)
        return total[0] + jnp.sum(z3, axis=0), total[1] + jnp.sum(z3 * z3, axis=0)

    def conv_a(r, rows=(0, 1, 2), first=0, pairs=w_out):
        parts = []
        for p in rows:
            for k in range(2):
                parts.append(img_t[r + p, pl.ds(k + first, pairs)].reshape(pairs * n_img, 2 * ch_a))
        w_val = wa_v[pl.ds(rows[0] * 4 * ch_a, len(rows) * 4 * ch_a)]
        return jnp.dot(jnp.concatenate(parts, axis=1), w_val, preferred_element_type=F32)

    def conv_down(r, first, count):
        m_val = count * n_img
        parts = [act_a[2 * r + p, pl.ds(first, count)].reshape(m_val, 2 * ch_a) for p in range(3)]
        parts += [act_a[2 * r + p, pl.ds(first + 1, count), :, 0:ch_a].reshape(m_val, ch_a) for p in range(3)]
        return jnp.dot(jnp.concatenate(parts, axis=1), wd_v[...], preferred_element_type=F32)

    def conv_b(r, layer, rows=(0, 1, 2), first=0, count=w_out):
        parts = []
        for p in rows:
            for q in range(3):
                parts.append(act_b[r + p, pl.ds(q + first, count)].reshape(count * n_img, ch_b))
        w_val = wb_v[layer, pl.ds(rows[0] * 3 * ch_b, len(rows) * 3 * ch_b)]
        return jnp.dot(jnp.concatenate(parts, axis=1), w_val, preferred_element_type=F32)

    def keep_z(r, z_val):
        zbuf[r] = z_val

    def keep_final(r, z_val, first=0):
        for x in range(z_val.shape[0] // n_img):
            for h in range(ch_b // 128):
                zfin[h, pl.ds((first + x) * n_img * n_out_row + r, n_img, stride=n_out_row), :] = (
                    z_val[x * n_img:(x + 1) * n_img, h * 128:(h + 1) * 128])

    def send_stats(layer, total):
        s1 = jnp.sum(total[0], axis=0, keepdims=True)
        s2 = jnp.sum(total[1], axis=0, keepdims=True)
        if layer == 0:
            s1 = s1[:, :ch_a] + s1[:, ch_a:]
            s2 = s2[:, :ch_a] + s2[:, ch_a:]
            s1 = jnp.concatenate([s1, s1], axis=1)
            s2 = jnp.concatenate([s2, s2], axis=1)
        both = jnp.concatenate([s1, s2], axis=0)
        stat_src[layer] = both
        last = layer == stat_src.shape[0] - 1
        slot = stat_out.at[me] if last else stat_dst.at[layer, me]
        if not last:
            stat_dst[layer, me] = both
        copies = []
        for i in range(1, n_group):
            copies.append(pltpu.make_async_remote_copy(
                src_ref=stat_src.at[layer], dst_ref=slot, send_sem=stat_send.at[layer],
                recv_sem=stat_recv.at[layer], device_id=peer(i), device_id_type=MESH))
        for c in copies:
            c.start()
        all_slots = (stat_out if last else stat_dst.at[layer]).at[pl.ds(0, n_group - 1)]
        waits = [pltpu.make_async_copy(all_slots, all_slots, sem.at[layer]) for sem in (stat_send, stat_recv)]
        if last:
            waits.append(pltpu.make_async_copy(stat_src.at[layer], slot, own_sem))
            waits[-1].start()
        return waits

    def finish_stats(layer, copies, gamma, beta, count):
        with jax.named_scope("stats_wait"):
            for c in copies:
                c.wait()
        tot = jnp.sum(stat_dst[layer], axis=0)
        mean = tot[0:1] / count
        var = tot[1:2] / count - mean * mean
        scale = gamma * lax.rsqrt(var + EPS_VALUE)
        return scale, beta - mean * scale

    def normalize(z_val, coef):
        scale, shift = coef
        return jnp.maximum(z_val * scale + shift, 0.0).astype(BF16)

    def z_row(layer, r):
        return 2 * r + (layer + 1) % 2

    zeros = (jnp.zeros((8, ch_b), F32), jnp.zeros((8, ch_b), F32))

    def t_body(r, carry):
        pltpu.make_async_copy(img.at[:, r], nat.at[r + 1], in_sem.at[r]).wait()
        transpose_row(r + 1)
        return carry

    with jax.named_scope("transpose"):
        lax.fori_loop(0, n_row, t_body, 0)
    wa_part = wa_v.at[pl.ds(0, 9 * ch_a)]
    pltpu.make_async_copy(wa_part, wa_part, w_sem.at[0]).wait()

    def a_rows(first, count, total):
        z_rows = [conv_a(first + j) for j in range(count)]
        for j in range(count):
            keep_z(first + j, z_rows[j])
            total = fold(total, z_rows[j])
        return total

    with jax.named_scope("barrier"):
        pl.semaphore_wait(barrier, n_group - 1)

    @pl.when(not_bottom)
    def _():
        for c in to_lower:
            c.start()

    @pl.when(not_top)
    def _():
        for c in to_upper:
            c.start()

    with jax.named_scope("conv_a_first"):
        total = a_rows(1, 1, zeros)
    with jax.named_scope("conv_a"):
        total = lax.fori_loop(0, (n_row - 4) // 2, lambda i, t: a_rows(2 + 2 * i, 2, t), total)
    with jax.named_scope("conv_a_part"):
        total = a_rows(n_row - 2, 1, total)
        keep_z(0, conv_a(0, (1, 2)))
        keep_z(n_row - 1, conv_a(n_row - 1, (0, 1)))

    pair_parts = ((0, (x_split - 1) // 2), ((x_split - 1) // 2, w_out - (x_split - 1) // 2))
    for k in range(2):
        with jax.named_scope("img_halo_wait"):
            @pl.when(not_top)
            def _():
                to_lower[k].wait_recv()

            @pl.when(not_bottom)
            def _():
                to_upper[k].wait_recv()

        with jax.named_scope("transpose_halo"):
            transpose_row(0, *x_parts[k])
            transpose_row(n_row + 1, *x_parts[k])
        with jax.named_scope("conv_a_edge"):
            first, count = pair_parts[k]
            rows = slice(first * n_img, (first + count) * n_img)
            for r, p in ((0, 0), (n_row - 1, 2)):
                z_val = conv_a(r, (p,), first, count) + zbuf[r, rows]
                zbuf[r, rows] = z_val
                total = fold(total, z_val)
    with jax.named_scope("send_stats"):
        copies = send_stats(0, total)

        @pl.when(not_top)
        def _():
            to_upper_z.start()

    pltpu.make_async_copy(wd_v, wd_v, w_sem.at[1]).wait()
    w_copies[-1].wait()
    with jax.named_scope("img_halo_wait2"):
        @pl.when(not_bottom)
        def _():
            to_upper[2].wait_recv()

    with jax.named_scope("conv_a_extra"):
        transpose_row(n_row + 2, 0, cols_x)
        zbuf[n_row, 0:n_pair * n_img] = conv_a(n_row, pairs=n_pair)
    n_a = float(n_group * n_img * n_row * width)
    wide = lambda v: jnp.concatenate([v, v], axis=1)
    coef_a = finish_stats(0, copies, wide(na[0, 0:1]), wide(na[0, 1:2]), n_a)

    n_piece = 3
    piece = w_out // n_piece

    def norm_a_cols(r, k):
        y_val = normalize(zbuf[r, k * piece * n_img:(k + 1) * piece * n_img], coef_a)
        act_a[r, pl.ds(k * piece, piece)] = y_val.reshape(piece, n_img, 2 * ch_a)

    def norm_a_row(r):
        for k in range(n_piece):
            norm_a_cols(r, k)

    def down_cols(r, k, total):
        z_val = conv_down(r, k * piece, piece)
        zbuf[z_row(0, r), k * piece * n_img:(k + 1) * piece * n_img] = z_val
        return fold(total, z_val)

    with jax.named_scope("conv_down"):
        total = zeros
        norm_a_row(0)

        @pl.when(not_top)
        def _():
            to_upper_y.start()

        for r in range(1, 3):
            norm_a_row(r)
        for r in range(n_out_row - 1):
            for k in range(n_piece):
                norm_a_cols(2 * r + 3, k)
                if 2 * r + 4 < n_row:
                    norm_a_cols(2 * r + 4, k)
                total = down_cols(r, k, total)
    with jax.named_scope("down_halo_wait"):
        @pl.when(not_top)
        def _():
            to_upper_z.wait_send()
            to_upper_y.wait_send()

        @pl.when(not_bottom)
        def _():
            to_upper_z.wait_recv()
            to_upper_y.wait_recv()

    with jax.named_scope("conv_down_last"):
        y_val = normalize(zbuf[n_row, 0:n_far * n_img], coef_a)
        y_val = jnp.where(is_bottom, jnp.zeros_like(y_val), y_val)
        act_a[n_row, pl.ds(0, n_far)] = y_val.reshape(n_far, n_img, 2 * ch_a)
        for k in range(n_piece):
            total = down_cols(n_out_row - 1, k, total)

    late_cols = (n_early, (n_early + 2 * w_out) // 3, w_out)
    last_row = n_out_row - 1

    def early_copies(layer):
        slot = layer % 2
        up = pltpu.make_async_remote_copy(
            src_ref=zbuf.at[z_row(layer, 0), pl.ds(0, n_early * n_img)], dst_ref=zhalo.at[slot, 1], send_sem=early_send.at[layer, 1],
            recv_sem=early_recv.at[layer, 1], device_id=upper, device_id_type=MESH)
        down = pltpu.make_async_remote_copy(
            src_ref=zbuf.at[z_row(layer, last_row), pl.ds(0, n_early * n_img)], dst_ref=zhalo.at[slot, 0], send_sem=early_send.at[layer, 0],
            recv_sem=early_recv.at[layer, 0], device_id=lower, device_id_type=MESH)
        return up, down

    def late_copies(layer, k):
        cols = pl.ds(1 + late_cols[k], late_cols[k + 1] - late_cols[k])
        up = pltpu.make_async_remote_copy(
            src_ref=act_b.at[1, cols], dst_ref=act_b.at[n_out_row + 1, cols],
            send_sem=halo_send.at[k, 1], recv_sem=halo_recv.at[k, 1], device_id=upper, device_id_type=MESH)
        down = pltpu.make_async_remote_copy(
            src_ref=act_b.at[n_out_row, cols], dst_ref=act_b.at[0, cols],
            send_sem=halo_send.at[k, 0], recv_sem=halo_recv.at[k, 0], device_id=lower, device_id_type=MESH)
        return up, down

    def start_both(up, down):
        @pl.when(not_top)
        def _():
            up.start()

        @pl.when(not_bottom)
        def _():
            down.start()

    n_b = float(n_group * m_row * n_out_row)
    with jax.named_scope("send_stats"):
        copies = send_stats(1, total)
        up_early, down_early = early_copies(0)
        start_both(up_early, down_early)
    coef = finish_stats(1, copies, nd[0:1], nd[1:2], n_b)

    for layer in range(n_layers_b):
        def norm_b_cols(r, first, count):
            z_val = zbuf[z_row(layer, r), pl.ds(first * n_img, count * n_img)]
            act_b[r + 1, pl.ds(1 + first, count)] = normalize(z_val, coef).reshape(count, n_img, ch_b)

        late = [late_copies(layer, k) for k in range(2)]
        with jax.named_scope("norm_edge"):
            for k in range(2):
                norm_b_cols(0, late_cols[k], late_cols[k + 1] - late_cols[k])
                norm_b_cols(last_row, late_cols[k], late_cols[k + 1] - late_cols[k])
                start_both(*late[k])

        last = layer == n_layers_b - 1
        def keep(r, z_val):
            if last:
                keep_final(r, z_val)
            else:
                zbuf[z_row(layer + 1, r)] = z_val

        with jax.named_scope("conv_b_main"):
            norm_b_cols(0, 0, n_early)
            norm_b_cols(last_row, 0, n_early)
            for r in range(1, last_row):
                norm_b_cols(r, 0, w_out)
            total = zeros
            zbuf[z_row(layer + 1, 0)] = conv_b(0, layer, (1, 2))
            for r in range(1, last_row):
                z_val = conv_b(r, layer)
                keep(r, z_val)
                total = fold(total, z_val)
            zbuf[z_row(layer + 1, last_row)] = conv_b(last_row, layer, (0, 1))

        def keep_edge(r, z_val, first):
            if last:
                keep_final(r, z_val, first)
            else:
                zbuf[z_row(layer + 1, r), first * n_img:first * n_img + z_val.shape[0]] = z_val

        def edge_cols(first, count, total):
            rows = slice(first * n_img, (first + count) * n_img)
            for r, p in ((0, 0), (last_row, 2)):
                z_val = conv_b(r, layer, (p,), first, count) + zbuf[z_row(layer + 1, r), rows]
                keep_edge(r, z_val, first)
                total = fold(total, z_val)
            return total

        with jax.named_scope("halo_wait"):
            def norm_halo(side, row):
                y_val = normalize(zhalo[layer % 2, side], coef)
                act_b[row, pl.ds(1, n_early)] = y_val.reshape(n_early, n_img, ch_b)

            @pl.when(not_top)
            def _():
                up_early.wait_send()
                down_early.wait_recv()
                norm_halo(0, 0)
                late[0][0].wait_send()
                late[0][1].wait_recv()

            @pl.when(not_bottom)
            def _():
                down_early.wait_send()
                up_early.wait_recv()
                norm_halo(1, n_out_row + 1)
                late[0][1].wait_send()
                late[0][0].wait_recv()

        split = late_cols[1] - 1
        with jax.named_scope("conv_b_edge"):
            total = edge_cols(0, split, total)
        with jax.named_scope("halo_wait2"):
            @pl.when(not_top)
            def _():
                late[1][0].wait_send()
                late[1][1].wait_recv()

            @pl.when(not_bottom)
            def _():
                late[1][1].wait_send()
                late[1][0].wait_recv()

        with jax.named_scope("conv_b_edge2"):
            total = edge_cols(split, w_out - split, total)

        with jax.named_scope("send_stats"):
            copies = send_stats(2 + layer, total)
            if not last:
                up_early, down_early = early_copies(layer + 1)
                start_both(up_early, down_early)
        if not last:
            coef = finish_stats(2 + layer, copies, nb[layer, 0:1], nb[layer, 1:2], n_b)

    with jax.named_scope("z_out"):
        z_copy = pltpu.make_async_copy(zfin, z_out, out_sem)
        z_copy.start()
        z_copy.wait()
    with jax.named_scope("last_stats_wait"):
        for c in copies:
            c.wait()

    @pl.when(not_bottom)
    def _():
        for c in to_lower:
            c.wait_send()

    @pl.when(not_top)
    def _():
        for c in to_upper:
            c.wait_send()


def finish_kernel(count, z_hbm, stat_hbm, norm_hbm, out, z_v, stat, norms, out_v, z_sem, small_sem, out_sem):
    n_img, w_out, n_out_row, ch_b = out.shape
    n_chunk = z_sem.shape[0]
    chunk = w_out // n_chunk
    per_col = n_img * n_out_row

    def z_copy(k):
        rows = pl.ds(k * chunk * per_col, chunk * per_col)
        return pltpu.make_async_copy(z_hbm.at[:, rows], z_v.at[:, rows], z_sem.at[k])

    def out_copy(k):
        cols = pl.ds(k * chunk, chunk)
        return pltpu.make_async_copy(out_v.at[:, cols], out.at[:, cols], out_sem.at[k])

    small = [pltpu.make_async_copy(stat_hbm, stat, small_sem.at[0]), pltpu.make_async_copy(norm_hbm, norms, small_sem.at[1])]
    for c in small:
        c.start()
    for k in range(n_chunk):
        z_copy(k).start(priority=1)
    for c in small:
        c.wait()
    norm = norms[norms.shape[0] - 1]
    tot = jnp.sum(stat[...], axis=0)
    mean = tot[0:1] / count
    var = tot[1:2] / count - mean * mean
    scale = norm[0:1] * lax.rsqrt(var + EPS_VALUE)
    shift = norm[1:2] - mean * scale
    for k in range(n_chunk):
        z_copy(k).wait()

        def out_body(x, carry):
            for h in range(ch_b // 128):
                lanes = slice(h * 128, (h + 1) * 128)
                z_val = z_v[h, pl.ds(x * per_col, per_col), :]
                y_val = jnp.maximum(z_val * scale[:, lanes] + shift[:, lanes], 0.0).astype(BF16)
                out_v[:, x, :, lanes] = y_val.reshape(n_img, n_out_row, 128)
            return carry

        lax.fori_loop(k * chunk, (k + 1) * chunk, out_body, 0, unroll=3)
        out_copy(k).start()
    for k in range(n_chunk):
        out_copy(k).wait()


def solution(mesh):
    n_sp, n_dp = mesh.shape['sp'], mesh.shape['dp']

    def local_stack(img, w_a, norm_a, w_down, norm_down, w_b, norm_b):
        n_img, n_row, width, ch_a = img.shape
        ch_b = w_down.shape[-1]
        n_out_row, w_out = n_row // 2, width // 2
        n_layers_b = w_b.shape[0]
        n_group = n_sp * n_dp
        any_spec = pl.BlockSpec(memory_space=pl.ANY)
        vmem_spec = pl.BlockSpec(memory_space=pltpu.VMEM)
        dma = pltpu.SemaphoreType.DMA
        n_stats = 2 + n_layers_b
        n_early = w_out // 4
        z_val, stats = pl.pallas_call(
            functools.partial(stack_kernel, n_dp, n_sp, n_early),
            out_shape=(
                jax.ShapeDtypeStruct((ch_b // 128, n_out_row * w_out * n_img, 128), F32),
                jax.ShapeDtypeStruct((n_group, 2, ch_b), F32),
            ),
            in_specs=[any_spec, any_spec, vmem_spec, any_spec, vmem_spec, any_spec, vmem_spec],
            out_specs=(any_spec, any_spec),
            scratch_shapes=[
                pltpu.VMEM((n_row + 3, n_img, width, ch_a), BF16),
                pltpu.VMEM((n_img * (width + 4), 128), F32),
                pltpu.VMEM((n_row + 3, w_out + 1, n_img, 2 * ch_a), BF16),
                pltpu.VMEM((n_row + 1, w_out + 1, n_img, 2 * ch_a), BF16),
                pltpu.VMEM((n_out_row + 2, w_out + 2, n_img, ch_b), BF16),
                pltpu.VMEM((n_row + 1, w_out * n_img, ch_b), F32),
                pltpu.VMEM((2, 2, n_early * n_img, ch_b), F32),
                pltpu.VMEM((ch_b // 128, n_out_row * w_out * n_img, 128), F32),
                pltpu.VMEM((12 * ch_a, ch_b), BF16),
                pltpu.VMEM((9 * ch_a, ch_b), BF16),
                pltpu.VMEM((n_layers_b, 9 * ch_b, ch_b), BF16),
                pltpu.VMEM((n_stats, 2, ch_b), F32),
                pltpu.VMEM((n_stats - 1, n_group, 2, ch_b), F32),
                dma((n_row,)), dma((3,)), dma((7,)), dma((7,)),
                dma((n_stats,)), dma((n_stats,)),
                dma((2, 2)), dma((2, 2)), dma((n_layers_b, 2)), dma((n_layers_b, 2)), dma, dma,
            ],
            compiler_params=pltpu.CompilerParams(
                collective_id=0, has_side_effects=True, vmem_limit_bytes=67043328),
        )(img, w_a[0], norm_a, w_down, norm_down, w_b.reshape(n_layers_b, 9 * ch_b, ch_b), norm_b)
        n_chunk = 4
        features = pl.pallas_call(
            functools.partial(finish_kernel, float(n_group * n_img * n_out_row * w_out)),
            out_shape=jax.ShapeDtypeStruct((n_img, w_out, n_out_row, ch_b), BF16),
            in_specs=[any_spec, any_spec, any_spec],
            out_specs=any_spec,
            scratch_shapes=[
                pltpu.VMEM(z_val.shape, F32),
                pltpu.VMEM(stats.shape, F32),
                pltpu.VMEM(norm_b.shape, F32),
                pltpu.VMEM((n_img, w_out, n_out_row, ch_b), BF16),
                dma((n_chunk,)), dma((2,)), dma((n_chunk,)),
            ],
            compiler_params=pltpu.CompilerParams(vmem_limit_bytes=67043328),
        )(z_val, stats, norm_b)
        return features.transpose(0, 2, 1, 3)

    act_spec = P(('pod', 'dp'), 'sp', None, None)
    return jax.shard_map(local_stack, mesh=mesh, in_specs=(act_spec, P(), P(), P(), P(), P(), P()), out_specs=act_spec, check_vma=False)
```

```python
import functools

import jax
import jax.numpy as jnp
from jax import lax
from jax.experimental import pallas as pl
from jax.experimental.pallas import tpu as pltpu
from jax.sharding import PartitionSpec as P

EPS_VALUE = 1e-5
MESH = pl.DeviceIdType.MESH
BF16 = jnp.bfloat16
F32 = jnp.float32


def stack_kernel(n_dp, n_sp, n_early, img, wa, na, wd, nd, wb, nb, z_out, stat_out,
                 nat, stage, img_t, act_a, act_b, zbuf, zhalo, zfin,
                 wa_v, wd_v, wb_v, stat_src, stat_dst,
                 in_sem, w_sem, halo_in_send, halo_in_recv, stat_send, stat_recv,
                 halo_send, halo_recv, early_send, early_recv, out_sem, own_sem):
    n_img, n_row, width, ch_a = img.shape
    n_out_row, w_out, ch_b = n_row // 2, width // 2, wd.shape[3]
    n_layers_b = wb.shape[0]
    n_group = n_dp * n_sp
    m_row = w_out * n_img
    my_pod, my_dp, my_sp = lax.axis_index("pod"), lax.axis_index("dp"), lax.axis_index("sp")
    me = my_dp * n_sp + my_sp
    is_top = my_sp == 0
    is_bottom = my_sp == n_sp - 1
    not_top = my_sp > 0
    not_bottom = my_sp < n_sp - 1
    upper = (my_pod, my_dp, lax.max(my_sp - 1, 0))
    lower = (my_pod, my_dp, lax.min(my_sp + 1, n_sp - 1))

    def peer(offset):
        flat = lax.rem(me + offset, n_group)
        return (my_pod, flat // n_sp, lax.rem(flat, n_sp))

    barrier = pltpu.get_barrier_semaphore()
    for i in range(1, n_group):
        pl.semaphore_signal(barrier, inc=1, device_id=peer(i), device_id_type=MESH)

    row_copies = [pltpu.make_async_copy(img.at[:, r], nat.at[r + 1], in_sem.at[r]) for r in range(n_row)]
    for c in row_copies:
        c.start()
    w_copies = []
    for p in range(3):
        for q in range(3):
            for half in range(2):
                k = q + half
                w_copies.append(pltpu.make_async_copy(
                    wa.at[p, q], wa_v.at[pl.ds(p * 4 * ch_a + k * ch_a, ch_a), pl.ds(half * ch_a, ch_a)],
                    w_sem.at[0]))
    for p in range(3):
        for q in range(3):
            off = p * 2 * ch_a + q * ch_a if q < 2 else 6 * ch_a + p * ch_a
            w_copies.append(pltpu.make_async_copy(wd.at[p, q], wd_v.at[pl.ds(off, ch_a)], w_sem.at[1]))
    w_copies.append(pltpu.make_async_copy(wb, wb_v, w_sem.at[2]))
    for c in w_copies:
        c.start()

    for p in range(3):
        wa_v[pl.ds(p * 4 * ch_a + 3 * ch_a, ch_a), 0:ch_a] = jnp.zeros((ch_a, ch_a), BF16)
        wa_v[pl.ds(p * 4 * ch_a, ch_a), ch_a:2 * ch_a] = jnp.zeros((ch_a, ch_a), BF16)
    n_rows_t = img_t.shape[0]
    img_t[:, 0, :, 0:ch_a] = jnp.zeros((n_rows_t, n_img, ch_a), BF16)
    img_t[:, w_out, :, ch_a:2 * ch_a] = jnp.zeros((n_rows_t, n_img, ch_a), BF16)
    act_a[:, w_out] = jnp.zeros((act_a.shape[0], n_img, 2 * ch_a), BF16)
    act_b[:, 0] = jnp.zeros((act_b.shape[0], n_img, ch_b), BF16)
    act_b[:, w_out + 1] = jnp.zeros((act_b.shape[0], n_img, ch_b), BF16)

    @pl.when(is_top)
    def _():
        nat[0] = jnp.zeros((n_img, width, ch_a), BF16)
        act_b[0] = jnp.zeros((w_out + 2, n_img, ch_b), BF16)

    @pl.when(is_bottom)
    def _():
        nat[n_row + 1] = jnp.zeros((n_img, width, ch_a), BF16)
        nat[n_row + 2] = jnp.zeros((n_img, width, ch_a), BF16)
        act_b[n_out_row + 1] = jnp.zeros((w_out + 2, n_img, ch_b), BF16)
        act_a[n_row] = jnp.zeros((w_out + 1, n_img, 2 * ch_a), BF16)

    x_split = width * 4 // 7 // 16 * 16
    cols_x = width * 10 // 21 // 16 * 16
    n_pair = cols_x // 2 - 1
    n_far = n_pair + w_out * 22 // 84

    def remote(src, dst, k, dev):
        return pltpu.make_async_remote_copy(
            src_ref=src, dst_ref=dst, send_sem=halo_in_send.at[k], recv_sem=halo_in_recv.at[k],
            device_id=dev, device_id_type=MESH)

    def image_halo(src_row, dst_row, dev, k, first, count):
        cols = pl.ds(first, count)
        return remote(nat.at[src_row + 1, :, cols], nat.at[dst_row, :, cols], k, dev)

    x_parts = ((0, x_split), (x_split, width - x_split))
    to_lower = [image_halo(n_row - 1, 0, lower, k, *x_parts[k]) for k in range(2)]
    to_upper = [image_halo(0, n_row + 1, upper, 2 + k, *x_parts[k]) for k in range(2)]
    to_upper.append(image_halo(1, n_row + 2, upper, 4, 0, cols_x))
    mid = pl.ds(n_pair * n_img, (n_far - n_pair) * n_img)
    to_upper_z = remote(zbuf.at[0, mid], zbuf.at[n_row, mid], 5, upper)
    far = pl.ds(n_far, w_out - n_far)
    to_upper_y = remote(act_a.at[0, far], act_a.at[n_row, far], 6, upper)

    def transpose_row(k, first=0, cols=width):
        pitch = stage.shape[0] // n_img

        for i in range(n_img):
            stage[pl.ds(i * pitch + first, cols), :] = nat[k, i, first:first + cols].astype(F32)
        for x in range(first, first + cols):
            half = (x + 1) % 2
            img_t[k, (x + 1) // 2, :, half * ch_a:(half + 1) * ch_a] = (
                stage[pl.ds(x, n_img, stride=pitch), :].astype(BF16))

    def fold(total, z_val):
        z3 = z_val.reshape(z_val.shape[0] // 8, 8, ch_b)
        return total[0] + jnp.sum(z3, axis=0), total[1] + jnp.sum(z3 * z3, axis=0)

    def conv_a(r, rows=(0, 1, 2), first=0, pairs=w_out):
        parts = []
        for p in rows:
            for k in range(2):
                parts.append(img_t[r + p, pl.ds(k + first, pairs)].reshape(pairs * n_img, 2 * ch_a))
        w_val = wa_v[pl.ds(rows[0] * 4 * ch_a, len(rows) * 4 * ch_a)]
        return jnp.dot(jnp.concatenate(parts, axis=1), w_val, preferred_element_type=F32)

    def conv_down(r, first, count):
        m_val = count * n_img
        parts = [act_a[2 * r + p, pl.ds(first, count)].reshape(m_val, 2 * ch_a) for p in range(3)]
        parts += [act_a[2 * r + p, pl.ds(first + 1, count), :, 0:ch_a].reshape(m_val, ch_a) for p in range(3)]
        return jnp.dot(jnp.concatenate(parts, axis=1), wd_v[...], preferred_element_type=F32)

    def conv_b(r, layer, rows=(0, 1, 2), first=0, count=w_out):
        parts = []
        for p in rows:
            for q in range(3):
                parts.append(act_b[r + p, pl.ds(q + first, count)].reshape(count * n_img, ch_b))
        w_val = wb_v[layer, pl.ds(rows[0] * 3 * ch_b, len(rows) * 3 * ch_b)]
        return jnp.dot(jnp.concatenate(parts, axis=1), w_val, preferred_element_type=F32)

    def keep_z(r, z_val):
        zbuf[r] = z_val

    def keep_final(r, z_val, first=0):
        for x in range(z_val.shape[0] // n_img):
            for h in range(ch_b // 128):
                zfin[h, pl.ds((first + x) * n_img * n_out_row + r, n_img, stride=n_out_row), :] = (
                    z_val[x * n_img:(x + 1) * n_img, h * 128:(h + 1) * 128])

    def send_stats(layer, total):
        s1 = jnp.sum(total[0], axis=0, keepdims=True)
        s2 = jnp.sum(total[1], axis=0, keepdims=True)
        if layer == 0:
            s1 = s1[:, :ch_a] + s1[:, ch_a:]
            s2 = s2[:, :ch_a] + s2[:, ch_a:]
            s1 = jnp.concatenate([s1, s1], axis=1)
            s2 = jnp.concatenate([s2, s2], axis=1)
        both = jnp.concatenate([s1, s2], axis=0)
        stat_src[layer] = both
        last = layer == stat_src.shape[0] - 1
        slot = stat_out.at[me] if last else stat_dst.at[layer, me]
        if not last:
            stat_dst[layer, me] = both
        copies = []
        for i in range(1, n_group):
            copies.append(pltpu.make_async_remote_copy(
                src_ref=stat_src.at[layer], dst_ref=slot, send_sem=stat_send.at[layer],
                recv_sem=stat_recv.at[layer], device_id=peer(i), device_id_type=MESH))
        for c in copies:
            c.start()
        all_slots = (stat_out if last else stat_dst.at[layer]).at[pl.ds(0, n_group - 1)]
        waits = [pltpu.make_async_copy(all_slots, all_slots, sem.at[layer]) for sem in (stat_send, stat_recv)]
        if last:
            waits.append(pltpu.make_async_copy(stat_src.at[layer], slot, own_sem))
            waits[-1].start()
        return waits

    def finish_stats(layer, copies, gamma, beta, count):
        with jax.named_scope("stats_wait"):
            for c in copies:
                c.wait()
        tot = jnp.sum(stat_dst[layer], axis=0)
        mean = tot[0:1] / count
        var = tot[1:2] / count - mean * mean
        scale = gamma * lax.rsqrt(var + EPS_VALUE)
        return scale, beta - mean * scale

    def normalize(z_val, coef):
        scale, shift = coef
        return jnp.maximum(z_val * scale + shift, 0.0).astype(BF16)

    def z_row(layer, r):
        return 2 * r + (layer + 1) % 2

    zeros = (jnp.zeros((8, ch_b), F32), jnp.zeros((8, ch_b), F32))

    def t_body(r, carry):
        pltpu.make_async_copy(img.at[:, r], nat.at[r + 1], in_sem.at[r]).wait()
        transpose_row(r + 1)
        return carry

    with jax.named_scope("transpose"):
        lax.fori_loop(0, n_row, t_body, 0)
    wa_part = wa_v.at[pl.ds(0, 9 * ch_a)]
    pltpu.make_async_copy(wa_part, wa_part, w_sem.at[0]).wait()

    def a_rows(first, count, total):
        z_rows = [conv_a(first + j) for j in range(count)]
        for j in range(count):
            keep_z(first + j, z_rows[j])
            total = fold(total, z_rows[j])
        return total

    with jax.named_scope("barrier"):
        pl.semaphore_wait(barrier, n_group - 1)

    @pl.when(not_bottom)
    def _():
        for c in to_lower:
            c.start()

    @pl.when(not_top)
    def _():
        for c in to_upper:
            c.start()

    with jax.named_scope("conv_a_first"):
        total = a_rows(1, 1, zeros)
    with jax.named_scope("conv_a"):
        total = lax.fori_loop(0, (n_row - 4) // 2, lambda i, t: a_rows(2 + 2 * i, 2, t), total)
    with jax.named_scope("conv_a_part"):
        total = a_rows(n_row - 2, 1, total)
        keep_z(0, conv_a(0, (1, 2)))
        keep_z(n_row - 1, conv_a(n_row - 1, (0, 1)))

    pair_parts = ((0, (x_split - 1) // 2), ((x_split - 1) // 2, w_out - (x_split - 1) // 2))
    for k in range(2):
        with jax.named_scope("img_halo_wait"):
            @pl.when(not_top)
            def _():
                to_lower[k].wait_recv()

            @pl.when(not_bottom)
            def _():
                to_upper[k].wait_recv()

        with jax.named_scope("transpose_halo"):
            transpose_row(0, *x_parts[k])
            transpose_row(n_row + 1, *x_parts[k])
        with jax.named_scope("conv_a_edge"):
            first, count = pair_parts[k]
            rows = slice(first * n_img, (first + count) * n_img)
            for r, p in ((0, 0), (n_row - 1, 2)):
                z_val = conv_a(r, (p,), first, count) + zbuf[r, rows]
                zbuf[r, rows] = z_val
                total = fold(total, z_val)
    with jax.named_scope("send_stats"):
        copies = send_stats(0, total)

        @pl.when(not_top)
        def _():
            to_upper_z.start()

    pltpu.make_async_copy(wd_v, wd_v, w_sem.at[1]).wait()
    w_copies[-1].wait()
    with jax.named_scope("img_halo_wait2"):
        @pl.when(not_bottom)
        def _():
            to_upper[2].wait_recv()

    with jax.named_scope("conv_a_extra"):
        transpose_row(n_row + 2, 0, cols_x)
        zbuf[n_row, 0:n_pair * n_img] = conv_a(n_row, pairs=n_pair)
    n_a = float(n_group * n_img * n_row * width)
    wide = lambda v: jnp.concatenate([v, v], axis=1)
    coef_a = finish_stats(0, copies, wide(na[0, 0:1]), wide(na[0, 1:2]), n_a)

    n_piece = 3
    piece = w_out // n_piece

    def norm_a_cols(r, k):
        y_val = normalize(zbuf[r, k * piece * n_img:(k + 1) * piece * n_img], coef_a)
        act_a[r, pl.ds(k * piece, piece)] = y_val.reshape(piece, n_img, 2 * ch_a)

    def norm_a_row(r):
        for k in range(n_piece):
            norm_a_cols(r, k)

    def down_cols(r, k, total):
        z_val = conv_down(r, k * piece, piece)
        zbuf[z_row(0, r), k * piece * n_img:(k + 1) * piece * n_img] = z_val
        return fold(total, z_val)

    with jax.named_scope("conv_down"):
        total = zeros
        norm_a_row(0)

        @pl.when(not_top)
        def _():
            to_upper_y.start()

        for r in range(1, 3):
            norm_a_row(r)
        for r in range(n_out_row - 1):
            for k in range(n_piece):
                norm_a_cols(2 * r + 3, k)
                if 2 * r + 4 < n_row:
                    norm_a_cols(2 * r + 4, k)
                total = down_cols(r, k, total)
    with jax.named_scope("down_halo_wait"):
        @pl.when(not_top)
        def _():
            to_upper_z.wait_send()
            to_upper_y.wait_send()

        @pl.when(not_bottom)
        def _():
            to_upper_z.wait_recv()
            to_upper_y.wait_recv()

    with jax.named_scope("conv_down_last"):
        y_val = normalize(zbuf[n_row, 0:n_far * n_img], coef_a)
        y_val = jnp.where(is_bottom, jnp.zeros_like(y_val), y_val)
        act_a[n_row, pl.ds(0, n_far)] = y_val.reshape(n_far, n_img, 2 * ch_a)
        for k in range(n_piece):
            total = down_cols(n_out_row - 1, k, total)

    late_cols = (n_early, (n_early + 3 * w_out) // 4, w_out)
    last_row = n_out_row - 1

    def early_copies(layer):
        slot = layer % 2
        up = pltpu.make_async_remote_copy(
            src_ref=zbuf.at[z_row(layer, 0), pl.ds(0, n_early * n_img)], dst_ref=zhalo.at[slot, 1], send_sem=early_send.at[layer, 1],
            recv_sem=early_recv.at[layer, 1], device_id=upper, device_id_type=MESH)
        down = pltpu.make_async_remote_copy(
            src_ref=zbuf.at[z_row(layer, last_row), pl.ds(0, n_early * n_img)], dst_ref=zhalo.at[slot, 0], send_sem=early_send.at[layer, 0],
            recv_sem=early_recv.at[layer, 0], device_id=lower, device_id_type=MESH)
        return up, down

    def late_copies(layer, k):
        cols = pl.ds(1 + late_cols[k], late_cols[k + 1] - late_cols[k])
        up = pltpu.make_async_remote_copy(
            src_ref=act_b.at[1, cols], dst_ref=act_b.at[n_out_row + 1, cols],
            send_sem=halo_send.at[k, 1], recv_sem=halo_recv.at[k, 1], device_id=upper, device_id_type=MESH)
        down = pltpu.make_async_remote_copy(
            src_ref=act_b.at[n_out_row, cols], dst_ref=act_b.at[0, cols],
            send_sem=halo_send.at[k, 0], recv_sem=halo_recv.at[k, 0], device_id=lower, device_id_type=MESH)
        return up, down

    def start_both(up, down):
        @pl.when(not_top)
        def _():
            up.start()

        @pl.when(not_bottom)
        def _():
            down.start()

    n_b = float(n_group * m_row * n_out_row)
    with jax.named_scope("send_stats"):
        copies = send_stats(1, total)
        up_early, down_early = early_copies(0)
        start_both(up_early, down_early)
    coef = finish_stats(1, copies, nd[0:1], nd[1:2], n_b)

    for layer in range(n_layers_b):
        def norm_b_cols(r, first, count):
            z_val = zbuf[z_row(layer, r), pl.ds(first * n_img, count * n_img)]
            act_b[r + 1, pl.ds(1 + first, count)] = normalize(z_val, coef).reshape(count, n_img, ch_b)

        late = [late_copies(layer, k) for k in range(2)]
        with jax.named_scope("norm_edge"):
            for k in range(2):
                norm_b_cols(0, late_cols[k], late_cols[k + 1] - late_cols[k])
                norm_b_cols(last_row, late_cols[k], late_cols[k + 1] - late_cols[k])
                start_both(*late[k])

        last = layer == n_layers_b - 1
        def keep(r, z_val):
            if last:
                keep_final(r, z_val)
            else:
                zbuf[z_row(layer + 1, r)] = z_val

        with jax.named_scope("conv_b_main"):
            norm_b_cols(0, 0, n_early)
            norm_b_cols(last_row, 0, n_early)
            for r in range(1, last_row):
                norm_b_cols(r, 0, w_out)
            total = zeros
            zbuf[z_row(layer + 1, 0)] = conv_b(0, layer, (1, 2))
            for r in range(1, last_row):
                z_val = conv_b(r, layer)
                keep(r, z_val)
                total = fold(total, z_val)
            zbuf[z_row(layer + 1, last_row)] = conv_b(last_row, layer, (0, 1))

        def keep_edge(r, z_val, first):
            if last:
                keep_final(r, z_val, first)
            else:
                zbuf[z_row(layer + 1, r), first * n_img:first * n_img + z_val.shape[0]] = z_val

        def edge_cols(first, count, total):
            rows = slice(first * n_img, (first + count) * n_img)
            for r, p in ((0, 0), (last_row, 2)):
                z_val = conv_b(r, layer, (p,), first, count) + zbuf[z_row(layer + 1, r), rows]
                keep_edge(r, z_val, first)
                total = fold(total, z_val)
            return total

        with jax.named_scope("halo_wait"):
            def norm_halo(side, row):
                y_val = normalize(zhalo[layer % 2, side], coef)
                act_b[row, pl.ds(1, n_early)] = y_val.reshape(n_early, n_img, ch_b)

            @pl.when(not_top)
            def _():
                up_early.wait_send()
                down_early.wait_recv()
                norm_halo(0, 0)
                late[0][0].wait_send()
                late[0][1].wait_recv()

            @pl.when(not_bottom)
            def _():
                down_early.wait_send()
                up_early.wait_recv()
                norm_halo(1, n_out_row + 1)
                late[0][1].wait_send()
                late[0][0].wait_recv()

        split = late_cols[1] - 1
        with jax.named_scope("conv_b_edge"):
            total = edge_cols(0, split, total)
        with jax.named_scope("halo_wait2"):
            @pl.when(not_top)
            def _():
                late[1][0].wait_send()
                late[1][1].wait_recv()

            @pl.when(not_bottom)
            def _():
                late[1][1].wait_send()
                late[1][0].wait_recv()

        with jax.named_scope("conv_b_edge2"):
            total = edge_cols(split, w_out - split, total)

        with jax.named_scope("send_stats"):
            copies = send_stats(2 + layer, total)
            if not last:
                up_early, down_early = early_copies(layer + 1)
                start_both(up_early, down_early)
        if not last:
            coef = finish_stats(2 + layer, copies, nb[layer, 0:1], nb[layer, 1:2], n_b)

    with jax.named_scope("z_out"):
        z_copy = pltpu.make_async_copy(zfin, z_out, out_sem)
        z_copy.start()
        z_copy.wait()
    with jax.named_scope("last_stats_wait"):
        for c in copies:
            c.wait()

    @pl.when(not_bottom)
    def _():
        for c in to_lower:
            c.wait_send()

    @pl.when(not_top)
    def _():
        for c in to_upper:
            c.wait_send()


def finish_kernel(count, z_hbm, stat_hbm, norm_hbm, out, z_v, stat, norms, out_v, z_sem, small_sem, out_sem):
    n_img, w_out, n_out_row, ch_b = out.shape
    n_chunk = z_sem.shape[0]
    chunk = w_out // n_chunk
    per_col = n_img * n_out_row

    def z_copy(k):
        rows = pl.ds(k * chunk * per_col, chunk * per_col)
        return pltpu.make_async_copy(z_hbm.at[:, rows], z_v.at[:, rows], z_sem.at[k])

    def out_copy(k):
        cols = pl.ds(k * chunk, chunk)
        return pltpu.make_async_copy(out_v.at[:, cols], out.at[:, cols], out_sem.at[k])

    small = [pltpu.make_async_copy(stat_hbm, stat, small_sem.at[0]), pltpu.make_async_copy(norm_hbm, norms, small_sem.at[1])]
    for c in small:
        c.start()
    for k in range(n_chunk):
        z_copy(k).start(priority=1)
    for c in small:
        c.wait()
    norm = norms[norms.shape[0] - 1]
    tot = jnp.sum(stat[...], axis=0)
    mean = tot[0:1] / count
    var = tot[1:2] / count - mean * mean
    scale = norm[0:1] * lax.rsqrt(var + EPS_VALUE)
    shift = norm[1:2] - mean * scale
    for k in range(n_chunk):
        z_copy(k).wait()

        def out_body(x, carry):
            for h in range(ch_b // 128):
                lanes = slice(h * 128, (h + 1) * 128)
                z_val = z_v[h, pl.ds(x * per_col, per_col), :]
                y_val = jnp.maximum(z_val * scale[:, lanes] + shift[:, lanes], 0.0).astype(BF16)
                out_v[:, x, :, lanes] = y_val.reshape(n_img, n_out_row, 128)
            return carry

        lax.fori_loop(k * chunk, (k + 1) * chunk, out_body, 0, unroll=7)
        out_copy(k).start()
    for k in range(n_chunk):
        out_copy(k).wait()


def solution(mesh):
    n_sp, n_dp = mesh.shape['sp'], mesh.shape['dp']

    def local_stack(img, w_a, norm_a, w_down, norm_down, w_b, norm_b):
        n_img, n_row, width, ch_a = img.shape
        ch_b = w_down.shape[-1]
        n_out_row, w_out = n_row // 2, width // 2
        n_layers_b = w_b.shape[0]
        n_group = n_sp * n_dp
        any_spec = pl.BlockSpec(memory_space=pl.ANY)
        vmem_spec = pl.BlockSpec(memory_space=pltpu.VMEM)
        dma = pltpu.SemaphoreType.DMA
        n_stats = 2 + n_layers_b
        n_early = w_out * 22 // 84
        z_val, stats = pl.pallas_call(
            functools.partial(stack_kernel, n_dp, n_sp, n_early),
            out_shape=(
                jax.ShapeDtypeStruct((ch_b // 128, n_out_row * w_out * n_img, 128), F32),
                jax.ShapeDtypeStruct((n_group, 2, ch_b), F32),
            ),
            in_specs=[any_spec, any_spec, vmem_spec, any_spec, vmem_spec, any_spec, vmem_spec],
            out_specs=(any_spec, any_spec),
            scratch_shapes=[
                pltpu.VMEM((n_row + 3, n_img, width, ch_a), BF16),
                pltpu.VMEM((n_img * (width + 4), 128), F32),
                pltpu.VMEM((n_row + 3, w_out + 1, n_img, 2 * ch_a), BF16),
                pltpu.VMEM((n_row + 1, w_out + 1, n_img, 2 * ch_a), BF16),
                pltpu.VMEM((n_out_row + 2, w_out + 2, n_img, ch_b), BF16),
                pltpu.VMEM((n_row + 1, w_out * n_img, ch_b), F32),
                pltpu.VMEM((2, 2, n_early * n_img, ch_b), F32),
                pltpu.VMEM((ch_b // 128, n_out_row * w_out * n_img, 128), F32),
                pltpu.VMEM((12 * ch_a, ch_b), BF16),
                pltpu.VMEM((9 * ch_a, ch_b), BF16),
                pltpu.VMEM((n_layers_b, 9 * ch_b, ch_b), BF16),
                pltpu.VMEM((n_stats, 2, ch_b), F32),
                pltpu.VMEM((n_stats - 1, n_group, 2, ch_b), F32),
                dma((n_row,)), dma((3,)), dma((7,)), dma((7,)),
                dma((n_stats,)), dma((n_stats,)),
                dma((2, 2)), dma((2, 2)), dma((n_layers_b, 2)), dma((n_layers_b, 2)), dma, dma,
            ],
            compiler_params=pltpu.CompilerParams(
                collective_id=0, has_side_effects=True, vmem_limit_bytes=67043328),
        )(img, w_a[0], norm_a, w_down, norm_down, w_b.reshape(n_layers_b, 9 * ch_b, ch_b), norm_b)
        n_chunk = 4
        features = pl.pallas_call(
            functools.partial(finish_kernel, float(n_group * n_img * n_out_row * w_out)),
            out_shape=jax.ShapeDtypeStruct((n_img, w_out, n_out_row, ch_b), BF16),
            in_specs=[any_spec, any_spec, any_spec],
            out_specs=any_spec,
            scratch_shapes=[
                pltpu.VMEM(z_val.shape, F32),
                pltpu.VMEM(stats.shape, F32),
                pltpu.VMEM(norm_b.shape, F32),
                pltpu.VMEM((n_img, w_out, n_out_row, ch_b), BF16),
                dma((n_chunk,)), dma((2,)), dma((n_chunk,)),
            ],
            compiler_params=pltpu.CompilerParams(vmem_limit_bytes=67043328),
        )(z_val, stats, norm_b)
        return features.transpose(0, 2, 1, 3)

    act_spec = P(('pod', 'dp'), 'sp', None, None)
    return jax.shard_map(local_stack, mesh=mesh, in_specs=(act_spec, P(), P(), P(), P(), P(), P()), out_specs=act_spec, check_vma=False)
```
